32 devices in a mesh: dp: 4 (over y, z), cp: 8 (over x, core).
Axes of the slice: x: 4, y: 2, z: 2, core: 2. Of those that a mesh axis runs over, the one named last changes fastest.
The devices are a block of a 4x4x8 slice.
Arguments:
- queries: bfloat16 [4, 2048, 32, 128], P('dp', 'cp'), parts along dimension 0
- keys: bfloat16 [4, 2048, 16, 128], P('dp', 'cp'), parts along dimension 0
- values: bfloat16 [4, 2048, 16, 128], P('dp', 'cp'), parts along dimension 0
- out_grad: bfloat16 [4, 2048, 32, 128], P('dp', 'cp'), parts along dimension 0
Outputs:
- output 1: bfloat16 [4, 2048, 32, 128], P('dp', 'cp'), parts along dimension 0
- output 2: float32 [4, 32, 2048], P('dp', None, 'cp'), parts along dimension 0
- output 3: bfloat16 [4, 2048, 32, 128], P('dp', 'cp'), parts along dimension 0
- output 4: bfloat16 [4, 2048, 16, 128], P('dp', 'cp'), parts along dimension 0
- output 5: bfloat16 [4, 2048, 16, 128], P('dp', 'cp'), parts along dimension 0
There are 4 independent parts. The reference program is written for one: setup_inputs(seed, part) draws one part's arguments, and reference() takes and returns one part's arrays. A program takes and returns all parts, laid end to end along the dimension named above; each array names one.
All inputs are finite; a program needn't handle non-finite values.
Results may differ from the reference program's by a relative error of at most 0.0193272.
Values are sent between devices in bfloat16 or wider.
A program may use at most 768 MiB of HBM per device.

```python
import jax
import jax.numpy as jnp
from jax import lax

BATCH = 1
SEQ = 2048
HEADS = 32
KV_HEADS = 16
HEAD = 128
QBLOCK = 128

RATIO = HEADS // KV_HEADS
SCALE = HEAD ** -0.5
NUM_BLOCKS = SEQ // QBLOCK


def setup_inputs(seed: int = 0, part: int = 0) -> dict:
    base_key = jax.random.fold_in(jax.random.key(seed), part)
    rng_keys = jax.random.split(base_key, 4)
    q_shape = (BATCH, SEQ, HEADS, HEAD)
    kv_shape = (BATCH, SEQ, KV_HEADS, HEAD)
    queries = jax.random.normal(rng_keys[0], q_shape, jnp.float32).astype(jnp.bfloat16)
    keys = jax.random.normal(rng_keys[1], kv_shape, jnp.float32).astype(jnp.bfloat16)
    values = jax.random.normal(rng_keys[2], kv_shape, jnp.float32).astype(jnp.bfloat16)
    out_grad = jax.random.normal(rng_keys[3], q_shape, jnp.float32).astype(jnp.bfloat16)
    return {"queries": queries, "keys": keys, "values": values, "out_grad": out_grad}


def reference(queries, keys, values, out_grad):
    keys_f = keys.astype(jnp.float32)
    values_f = values.astype(jnp.float32)
    key_pos = jnp.arange(SEQ)
    query_blocks = jnp.moveaxis(queries.reshape(BATCH, NUM_BLOCKS, QBLOCK, KV_HEADS, RATIO, HEAD), 1, 0)
    grad_blocks = jnp.moveaxis(out_grad.reshape(BATCH, NUM_BLOCKS, QBLOCK, KV_HEADS, RATIO, HEAD), 1, 0)

    def block_step(carry, block_in):
        grad_key, grad_value = carry
        block_idx, query_blk, grad_blk = block_in
        query_f = query_blk.astype(jnp.float32)
        grad_f = grad_blk.astype(jnp.float32)
        query_pos = block_idx * QBLOCK + jnp.arange(QBLOCK)
        causal = query_pos[:, None] >= key_pos[None, :]
        scores = jnp.einsum("bqgrd,bkgd->bgrqk", query_f, keys_f) * SCALE
        scores = jnp.where(causal, scores, -jnp.inf)
        row_max = jnp.max(scores, axis=-1, keepdims=True)
        row_lse = row_max + jnp.log(jnp.sum(jnp.exp(scores - row_max), axis=-1, keepdims=True))
        prob_mat = jnp.exp(scores - row_lse)
        prob_round = prob_mat.astype(jnp.bfloat16).astype(jnp.float32)
        out_blk = jnp.einsum("bgrqk,bkgd->bqgrd", prob_round, values_f).astype(jnp.bfloat16)
        delta = jnp.einsum("bqgrd,bqgrd->bgrq", grad_f, out_blk.astype(jnp.float32))
        grad_prob = jnp.einsum("bqgrd,bkgd->bgrqk", grad_f, values_f)
        grad_score = prob_mat * (grad_prob - delta[..., None])
        score_round = grad_score.astype(jnp.bfloat16).astype(jnp.float32)
        grad_query = jnp.einsum("bgrqk,bkgd->bqgrd", score_round, keys_f) * SCALE
        grad_key = grad_key + jnp.einsum("bgrqk,bqgrd->bkgd", score_round, query_f) * SCALE
        grad_value = grad_value + jnp.einsum("bgrqk,bqgrd->bkgd", prob_round, grad_f)
        return (grad_key, grad_value), (out_blk, row_lse[..., 0], grad_query.astype(jnp.bfloat16))

    zero_kv = jnp.zeros((BATCH, SEQ, KV_HEADS, HEAD), jnp.float32)
    carry_out, block_outs = lax.scan(block_step, (zero_kv, zero_kv), (jnp.arange(NUM_BLOCKS), query_blocks, grad_blocks))
    out_blocks, lse_blocks, dq_blocks = block_outs
    attn_out = jnp.moveaxis(out_blocks, 0, 1).reshape(BATCH, SEQ, HEADS, HEAD)
    row_lse = jnp.moveaxis(lse_blocks, 0, 3).reshape(BATCH, HEADS, SEQ)
    grad_query = jnp.moveaxis(dq_blocks, 0, 1).reshape(BATCH, SEQ, HEADS, HEAD)
    grad_key = carry_out[0].astype(jnp.bfloat16)
    grad_value = carry_out[1].astype(jnp.bfloat16)
    return attn_out, row_lse, grad_query, grad_key, grad_value
```

```python
import functools

import jax
import jax.numpy as jnp
from jax import lax
from jax.experimental import pallas as pl
from jax.experimental.pallas import tpu as pltpu
from jax.sharding import PartitionSpec as P

MESH = pl.DeviceIdType.MESH
F32 = jnp.float32
BF16 = jnp.bfloat16
NT = (((1,), (1,)), ((), ()))


def attention_kernel(n, groups, ratio, tokens, dim, q_in, k_in, v_in, g_in, o_out, dq_out, dk_out, dv_out, lse_out, qb, kb, vb, gb, ob, dqb, dkb, dvb, lseb, s_scr, dk_acc, dv_acc, kt, vt, t_scr, in_send, in_recv, out_send, out_recv, lse_send, lse_recv, in_local, out_local, lse_local):
    me = lax.axis_index("cp")
    scale = dim ** -0.5
    wide = ratio * dim

    def peer(offset):
        return {"cp": lax.rem(me + offset, n)}

    def row_of(device):
        return pl.ds(pl.multiple_of(device * tokens, tokens), tokens)

    def column_of(head, width):
        return pl.ds(pl.multiple_of(head * width, width), width)

    barrier = pltpu.get_barrier_semaphore()
    for offset in range(1, n):
        pl.semaphore_signal(barrier, inc=1, device_id=peer(offset), device_id_type=MESH)
    pl.semaphore_wait(barrier, n - 1)

    in_arrays = ((k_in, kb, dim), (v_in, vb, dim), (q_in, qb, wide), (g_in, gb, wide))
    in_copies = {}
    for g in range(groups):
        for offset in range(1, n):
            target = lax.rem(me + offset, n)
            for a, (src, dst, width) in enumerate(in_arrays):
                copy = pltpu.make_async_remote_copy(
                    src_ref=src.at[:, column_of(target * groups + g, width)],
                    dst_ref=dst.at[g, row_of(me)],
                    send_sem=in_send.at[g, offset - 1, a],
                    recv_sem=in_recv.at[g, offset - 1, a],
                    device_id=peer(offset),
                    device_id_type=MESH,
                )
                copy.start()
                in_copies[g, offset, a] = copy
        for a, (src, dst, width) in enumerate(in_arrays):
            copy = pltpu.make_async_copy(src.at[:, column_of(me * groups + g, width)], dst.at[g, row_of(me)], in_local.at[g, a])
            copy.start()
            in_copies[g, 0, a] = copy

    key_pos = lax.broadcasted_iota(jnp.int32, (tokens, tokens), 0)
    query_pos = lax.broadcasted_iota(jnp.int32, (tokens, tokens), 1)

    def fold(x, op):
        return op(x.reshape(tokens // 8, 8, tokens), axis=0)

    def head_compute(g):
        def prepare(j, _):
            rows = row_of(j)
            kt[:, rows] = jnp.transpose(kb[g, rows, :].astype(F32)).astype(BF16)
            vt[:, rows] = jnp.transpose(vb[g, rows, :].astype(F32)).astype(BF16)
            dk_acc[rows, :] = jnp.zeros((tokens, dim), F32)
            dv_acc[rows, :] = jnp.zeros((tokens, dim), F32)
            return 0

        lax.fori_loop(0, n, prepare, 0)

        def block(i, _):
            rows_i = row_of(i)
            qs = [qb[g, rows_i, r * dim:(r + 1) * dim] for r in range(ratio)]
            gs = [gb[g, rows_i, r * dim:(r + 1) * dim] for r in range(ratio)]

            def score(j, maxes):
                rows = row_of(j)
                key_blk = kb[g, rows, :]
                new = []
                for r in range(ratio):
                    s = lax.dot_general(key_blk, qs[r], NT, preferred_element_type=F32)
                    s_scr[r, rows, :] = s
                    new.append(jnp.maximum(maxes[r], fold(s, jnp.max)))
                return tuple(new)

            maxes = lax.fori_loop(0, i, score, tuple(jnp.full((8, tokens), -jnp.inf, F32) for _ in range(ratio)))
            key_blk = kb[g, rows_i, :]
            tops = []
            for r in range(ratio):
                s = lax.dot_general(key_blk, qs[r], NT, preferred_element_type=F32)
                s = jnp.where(key_pos <= query_pos, s, -jnp.inf)
                s_scr[r, rows_i, :] = s
                tops.append(jnp.max(jnp.maximum(maxes[r], fold(s, jnp.max)), axis=0, keepdims=True))

            def weigh(j, sums):
                rows = row_of(j)
                new = []
                for r in range(ratio):
                    p = jnp.exp((s_scr[r, rows, :] - tops[r]) * scale)
                    s_scr[r, rows, :] = p
                    new.append(sums[r] + fold(p, jnp.sum))
                return tuple(new)

            sums = lax.fori_loop(0, i + 1, weigh, tuple(jnp.zeros((8, tokens), F32) for _ in range(ratio)))
            totals = [jnp.sum(x, axis=0, keepdims=True) for x in sums]
            invs = [1.0 / x for x in totals]
            for r in range(ratio):
                lseb[i, pl.ds(g * ratio + r, 1), :] = tops[r] * scale + jnp.log(totals[r])
                t_scr[r] = jnp.zeros((dim, tokens), F32)

            def outputs(j, _):
                rows = row_of(j)
                vt_blk = vt[:, rows]
                dv_new = dv_acc[rows, :]
                for r in range(ratio):
                    p_low = (s_scr[r, rows, :] * invs[r]).astype(BF16)
                    t_scr[r] += jnp.dot(vt_blk, p_low, preferred_element_type=F32)
                    dv_new += jnp.dot(p_low, gs[r], preferred_element_type=F32)
                dv_acc[rows, :] = dv_new
                return 0

            lax.fori_loop(0, i + 1, outputs, 0)
            deltas = []
            for r in range(ratio):
                out = jnp.transpose(t_scr[r]).astype(BF16)
                ob[g, rows_i, r * dim:(r + 1) * dim] = out
                deltas.append(jnp.sum(jnp.transpose(gs[r].astype(F32) * out.astype(F32)), axis=0, keepdims=True))
            for r in range(ratio):
                t_scr[r] = jnp.zeros((dim, tokens), F32)

            def gradients(j, _):
                rows = row_of(j)
                kt_blk = kt[:, rows]
                value_blk = vb[g, rows, :]
                dk_new = dk_acc[rows, :]
                for r in range(ratio):
                    dp = lax.dot_general(value_blk, gs[r], NT, preferred_element_type=F32)
                    ds = ((s_scr[r, rows, :] * invs[r]) * (dp - deltas[r])).astype(BF16)
                    t_scr[r] += jnp.dot(kt_blk, ds, preferred_element_type=F32)
                    dk_new += jnp.dot(ds, qs[r], preferred_element_type=F32)
                dk_acc[rows, :] = dk_new
                return 0

            lax.fori_loop(0, i + 1, gradients, 0)
            for r in range(ratio):
                dqb[g, rows_i, r * dim:(r + 1) * dim] = jnp.transpose(t_scr[r] * scale).astype(BF16)
            return 0

        lax.fori_loop(0, n, block, 0)

        def finish(j, _):
            rows = row_of(j)
            dkb[g, rows, :] = (dk_acc[rows, :] * scale).astype(BF16)
            dvb[g, rows, :] = dv_acc[rows, :].astype(BF16)
            return 0

        lax.fori_loop(0, n, finish, 0)

    out_arrays = ((ob, o_out, wide), (dqb, dq_out, wide), (dkb, dk_out, dim), (dvb, dv_out, dim))
    out_copies = {}
    for g in range(groups):
        for offset in range(n):
            for a in range(4):
                if offset:
                    in_copies[g, offset, a].wait_recv()
                else:
                    in_copies[g, offset, a].wait()
        head_compute(g)
        for offset in range(1, n):
            target = lax.rem(me + offset, n)
            for a, (src, dst, width) in enumerate(out_arrays):
                copy = pltpu.make_async_remote_copy(
                    src_ref=src.at[g, row_of(target)],
                    dst_ref=dst.at[:, column_of(me * groups + g, width)],
                    send_sem=out_send.at[g, offset - 1, a],
                    recv_sem=out_recv.at[g, offset - 1, a],
                    device_id=peer(offset),
                    device_id_type=MESH,
                )
                copy.start()
                out_copies[g, offset, a] = copy
        for a, (src, dst, width) in enumerate(out_arrays):
            copy = pltpu.make_async_copy(src.at[g, row_of(me)], dst.at[:, column_of(me * groups + g, width)], out_local.at[g, a])
            copy.start()
            out_copies[g, 0, a] = copy

    lse_copies = []
    for offset in range(1, n):
        target = lax.rem(me + offset, n)
        copy = pltpu.make_async_remote_copy(
            src_ref=lseb.at[target],
            dst_ref=lse_out.at[me],
            send_sem=lse_send.at[offset - 1],
            recv_sem=lse_recv.at[offset - 1],
            device_id=peer(offset),
            device_id_type=MESH,
        )
        copy.start()
        lse_copies.append(copy)
    copy = pltpu.make_async_copy(lseb.at[me], lse_out.at[me], lse_local)
    copy.start()
    lse_copies.append(copy)

    for (g, offset, a), copy in in_copies.items():
        if offset:
            copy.wait_send()
    for copy in out_copies.values():
        copy.wait()
    for copy in lse_copies:
        copy.wait()


def solution(mesh):
    n = mesh.shape["cp"]

    def attention_shard(queries, keys, values, out_grad):
        batch, tokens, heads, dim = queries.shape
        kv_heads = keys.shape[2]
        ratio = heads // kv_heads
        groups = kv_heads // n
        total = n * tokens
        wide = ratio * dim
        stats = -(-groups * ratio // 8) * 8

        def flat(x):
            return x.reshape(tokens, x.shape[2] * dim)

        any_space = pl.BlockSpec(memory_space=pl.ANY)
        dma = pltpu.SemaphoreType.DMA
        out, dq, dk, dv, lse = pl.pallas_call(
            functools.partial(attention_kernel, n, groups, ratio, tokens, dim),
            out_shape=(
                jax.ShapeDtypeStruct((tokens, heads * dim), BF16),
                jax.ShapeDtypeStruct((tokens, heads * dim), BF16),
                jax.ShapeDtypeStruct((tokens, kv_heads * dim), BF16),
                jax.ShapeDtypeStruct((tokens, kv_heads * dim), BF16),
                jax.ShapeDtypeStruct((n, stats, tokens), F32),
            ),
            in_specs=[any_space] * 4,
            out_specs=(any_space,) * 5,
            scratch_shapes=[
                pltpu.VMEM((groups, total, wide), BF16),
                pltpu.VMEM((groups, total, dim), BF16),
                pltpu.VMEM((groups, total, dim), BF16),
                pltpu.VMEM((groups, total, wide), BF16),
                pltpu.VMEM((groups, total, wide), BF16),
                pltpu.VMEM((groups, total, wide), BF16),
                pltpu.VMEM((groups, total, dim), BF16),
                pltpu.VMEM((groups, total, dim), BF16),
                pltpu.VMEM((n, stats, tokens), F32),
                pltpu.VMEM((ratio, total, tokens), F32),
                pltpu.VMEM((total, dim), F32),
                pltpu.VMEM((total, dim), F32),
                pltpu.VMEM((dim, total), BF16),
                pltpu.VMEM((dim, total), BF16),
                pltpu.VMEM((ratio, dim, tokens), F32),
                dma((groups, n - 1, 4)),
                dma((groups, n - 1, 4)),
                dma((groups, n - 1, 4)),
                dma((groups, n - 1, 4)),
                dma((n - 1,)),
                dma((n - 1,)),
                dma((groups, 4)),
                dma((groups, 4)),
                dma,
            ],
            compiler_params=pltpu.CompilerParams(collective_id=0, has_side_effects=True, vmem_limit_bytes=60 * 2**20),
            name="heads_attention",
        )(flat(queries), flat(keys), flat(values), flat(out_grad))
        shape = (batch, tokens, heads, dim)
        kv_shape = (batch, tokens, kv_heads, dim)
        row_lse = lse[:, :groups * ratio, :].reshape(batch, heads, tokens)
        return out.reshape(shape), row_lse, dq.reshape(shape), dk.reshape(kv_shape), dv.reshape(kv_shape)

    seq_spec = P("dp", "cp")
    return jax.shard_map(attention_shard, mesh=mesh, in_specs=(seq_spec,) * 4, out_specs=(seq_spec, P("dp", None, "cp"), seq_spec, seq_spec, seq_spec), check_vma=False)
```

```python
import functools

import jax
import jax.numpy as jnp
from jax import lax
from jax.experimental import pallas as pl
from jax.experimental.pallas import tpu as pltpu
from jax.sharding import PartitionSpec as P

MESH = pl.DeviceIdType.MESH
F32 = jnp.float32
BF16 = jnp.bfloat16
NT = (((1,), (1,)), ((), ()))


def attention_kernel(n, groups, ratio, tokens, dim, q_in, k_in, v_in, g_in, o_out, dq_out, dk_out, dv_out, lse_out, qb, kb, vb, gb, ob, dqb, dkb, dvb, lseb, s_scr, dk_acc, dv_acc, kt, vt, t_scr, q_cat, g_cat, in_send, in_recv, out_send, out_recv, lse_send, lse_recv, in_local, out_local, lse_local):
    me = lax.axis_index("cp")
    scale = dim ** -0.5
    wide = ratio * dim

    def peer(offset):
        return {"cp": lax.rem(me + offset, n)}

    def row_of(device):
        return pl.ds(pl.multiple_of(device * tokens, tokens), tokens)

    def column_of(head, width):
        return pl.ds(pl.multiple_of(head * width, width), width)

    barrier = pltpu.get_barrier_semaphore()
    for offset in range(1, n):
        pl.semaphore_signal(barrier, inc=1, device_id=peer(offset), device_id_type=MESH)
    pl.semaphore_wait(barrier, n - 1)

    in_arrays = ((k_in, kb, dim), (v_in, vb, dim), (q_in, qb, wide), (g_in, gb, wide))
    in_copies = {}
    for g in range(groups):
        for offset in range(1, n):
            target = lax.rem(me + offset, n)
            for a, (src, dst, width) in enumerate(in_arrays):
                copy = pltpu.make_async_remote_copy(
                    src_ref=src.at[:, column_of(target * groups + g, width)],
                    dst_ref=dst.at[g, row_of(me)],
                    send_sem=in_send.at[g, offset - 1, a],
                    recv_sem=in_recv.at[g, offset - 1, a],
                    device_id=peer(offset),
                    device_id_type=MESH,
                )
                copy.start()
                in_copies[g, offset, a] = copy
        for a, (src, dst, width) in enumerate(in_arrays):
            copy = pltpu.make_async_copy(src.at[:, column_of(me * groups + g, width)], dst.at[g, row_of(me)], in_local.at[g, a])
            copy.start()
            in_copies[g, 0, a] = copy

    blk = q_cat.shape[0] // ratio
    cols = ratio * blk
    key_pos = lax.broadcasted_iota(jnp.int32, (blk, blk), 0)
    query_pos = lax.broadcasted_iota(jnp.int32, (blk, blk), 1)

    def fold(x, op):
        return op(x.reshape(blk // 8, 8, cols), axis=0)

    def block_of(index):
        return pl.ds(pl.multiple_of(index * blk, blk), blk)

    def head_compute(g):
        def prepare(j, _):
            rows = block_of(j)
            kt[:, rows] = jnp.transpose(kb[g, rows, :].astype(F32)).astype(BF16)
            vt[:, rows] = jnp.transpose(vb[g, rows, :].astype(F32)).astype(BF16)
            dk_acc[rows, :] = jnp.zeros((blk, dim), F32)
            dv_acc[rows, :] = jnp.zeros((blk, dim), F32)
            return 0

        lax.fori_loop(0, n * tokens // blk, prepare, 0)

        def block(i, _):
            rows_i = block_of(i)
            for r in range(ratio):
                q_cat[r * blk:(r + 1) * blk, :] = qb[g, rows_i, r * dim:(r + 1) * dim]
                g_cat[r * blk:(r + 1) * blk, :] = gb[g, rows_i, r * dim:(r + 1) * dim]

            def score(j, top):
                rows = block_of(j)
                s = lax.dot_general(kb[g, rows, :], q_cat[...], NT, preferred_element_type=F32)
                s_scr[rows, :] = s
                return jnp.maximum(top, fold(s, jnp.max))

            top = lax.fori_loop(0, i, score, jnp.full((8, cols), -jnp.inf, F32))
            s = lax.dot_general(kb[g, rows_i, :], q_cat[...], NT, preferred_element_type=F32)
            keep = jnp.concatenate([key_pos <= query_pos] * ratio, axis=1)
            s = jnp.where(keep, s, -jnp.inf)
            s_scr[rows_i, :] = s
            top = jnp.max(jnp.maximum(top, fold(s, jnp.max)), axis=0, keepdims=True)

            def weigh(j, total):
                rows = block_of(j)
                p = jnp.exp((s_scr[rows, :] - top) * scale)
                s_scr[rows, :] = p
                return total + fold(p, jnp.sum)

            total = lax.fori_loop(0, i + 1, weigh, jnp.zeros((8, cols), F32))
            total = jnp.sum(total, axis=0, keepdims=True)
            inv = 1.0 / total
            lse = top * scale + jnp.log(total)
            for r in range(ratio):
                for t in range(blk // tokens):
                    at = r * blk + t * tokens
                    lseb[i * (blk // tokens) + t, pl.ds(g * ratio + r, 1), :] = lse[:, at:at + tokens]
            t_scr[...] = jnp.zeros((dim, cols), F32)

            def outputs(j, _):
                rows = block_of(j)
                p_low = (s_scr[rows, :] * inv).astype(BF16)
                t_scr[...] += jnp.dot(vt[:, rows], p_low, preferred_element_type=F32)
                dv_acc[rows, :] += jnp.dot(p_low, g_cat[...], preferred_element_type=F32)
                return 0

            lax.fori_loop(0, i + 1, outputs, 0)
            out = jnp.transpose(t_scr[...]).astype(BF16)
            for r in range(ratio):
                ob[g, rows_i, r * dim:(r + 1) * dim] = out[r * blk:(r + 1) * blk]
            delta = jnp.sum(jnp.transpose(g_cat[...].astype(F32) * out.astype(F32)), axis=0, keepdims=True)
            t_scr[...] = jnp.zeros((dim, cols), F32)

            def gradients(j, _):
                rows = block_of(j)
                dp = lax.dot_general(vb[g, rows, :], g_cat[...], NT, preferred_element_type=F32)
                ds = ((s_scr[rows, :] * inv) * (dp - delta)).astype(BF16)
                t_scr[...] += jnp.dot(kt[:, rows], ds, preferred_element_type=F32)
                dk_acc[rows, :] += jnp.dot(ds, q_cat[...], preferred_element_type=F32)
                return 0

            lax.fori_loop(0, i + 1, gradients, 0)
            dq = jnp.transpose(t_scr[...] * scale).astype(BF16)
            for r in range(ratio):
                dqb[g, rows_i, r * dim:(r + 1) * dim] = dq[r * blk:(r + 1) * blk]
            return 0

        lax.fori_loop(0, n * tokens // blk, block, 0)

        def finish(j, _):
            rows = block_of(j)
            dkb[g, rows, :] = (dk_acc[rows, :] * scale).astype(BF16)
            dvb[g, rows, :] = dv_acc[rows, :].astype(BF16)
            return 0

        lax.fori_loop(0, n * tokens // blk, finish, 0)

    out_arrays = ((ob, o_out, wide), (dqb, dq_out, wide), (dkb, dk_out, dim), (dvb, dv_out, dim))
    out_copies = {}
    for g in range(groups):
        for offset in range(n):
            for a in range(4):
                if offset:
                    in_copies[g, offset, a].wait_recv()
                else:
                    in_copies[g, offset, a].wait()
        head_compute(g)
        for offset in range(1, n):
            target = lax.rem(me + offset, n)
            for a, (src, dst, width) in enumerate(out_arrays):
                copy = pltpu.make_async_remote_copy(
                    src_ref=src.at[g, row_of(target)],
                    dst_ref=dst.at[:, column_of(me * groups + g, width)],
                    send_sem=out_send.at[g, offset - 1, a],
                    recv_sem=out_recv.at[g, offset - 1, a],
                    device_id=peer(offset),
                    device_id_type=MESH,
                )
                copy.start()
                out_copies[g, offset, a] = copy
        for a, (src, dst, width) in enumerate(out_arrays):
            copy = pltpu.make_async_copy(src.at[g, row_of(me)], dst.at[:, column_of(me * groups + g, width)], out_local.at[g, a])
            copy.start()
            out_copies[g, 0, a] = copy

    lse_copies = []
    for offset in range(1, n):
        target = lax.rem(me + offset, n)
        copy = pltpu.make_async_remote_copy(
            src_ref=lseb.at[target],
            dst_ref=lse_out.at[me],
            send_sem=lse_send.at[offset - 1],
            recv_sem=lse_recv.at[offset - 1],
            device_id=peer(offset),
            device_id_type=MESH,
        )
        copy.start()
        lse_copies.append(copy)
    copy = pltpu.make_async_copy(lseb.at[me], lse_out.at[me], lse_local)
    copy.start()
    lse_copies.append(copy)

    for (g, offset, a), copy in in_copies.items():
        if offset:
            copy.wait_send()
    for copy in out_copies.values():
        copy.wait()
    for copy in lse_copies:
        copy.wait()


def solution(mesh):
    n = mesh.shape["cp"]

    def attention_shard(queries, keys, values, out_grad):
        batch, tokens, heads, dim = queries.shape
        kv_heads = keys.shape[2]
        ratio = heads // kv_heads
        groups = kv_heads // n
        total = n * tokens
        wide = ratio * dim
        blk = 2 * tokens
        stats = -(-groups * ratio // 8) * 8

        def flat(x):
            return x.reshape(tokens, x.shape[2] * dim)

        any_space = pl.BlockSpec(memory_space=pl.ANY)
        dma = pltpu.SemaphoreType.DMA
        out, dq, dk, dv, lse = pl.pallas_call(
            functools.partial(attention_kernel, n, groups, ratio, tokens, dim),
            out_shape=(
                jax.ShapeDtypeStruct((tokens, heads * dim), BF16),
                jax.ShapeDtypeStruct((tokens, heads * dim), BF16),
                jax.ShapeDtypeStruct((tokens, kv_heads * dim), BF16),
                jax.ShapeDtypeStruct((tokens, kv_heads * dim), BF16),
                jax.ShapeDtypeStruct((n, stats, tokens), F32),
            ),
            in_specs=[any_space] * 4,
            out_specs=(any_space,) * 5,
            scratch_shapes=[
                pltpu.VMEM((groups, total, wide), BF16),
                pltpu.VMEM((groups, total, dim), BF16),
                pltpu.VMEM((groups, total, dim), BF16),
                pltpu.VMEM((groups, total, wide), BF16),
                pltpu.VMEM((groups, total, wide), BF16),
                pltpu.VMEM((groups, total, wide), BF16),
                pltpu.VMEM((groups, total, dim), BF16),
                pltpu.VMEM((groups, total, dim), BF16),
                pltpu.VMEM((n, stats, tokens), F32),
                pltpu.VMEM((total, ratio * blk), F32),
                pltpu.VMEM((total, dim), F32),
                pltpu.VMEM((total, dim), F32),
                pltpu.VMEM((dim, total), BF16),
                pltpu.VMEM((dim, total), BF16),
                pltpu.VMEM((dim, ratio * blk), F32),
                pltpu.VMEM((ratio * blk, dim), BF16),
                pltpu.VMEM((ratio * blk, dim), BF16),
                dma((groups, n - 1, 4)),
                dma((groups, n - 1, 4)),
                dma((groups, n - 1, 4)),
                dma((groups, n - 1, 4)),
                dma((n - 1,)),
                dma((n - 1,)),
                dma((groups, 4)),
                dma((groups, 4)),
                dma,
            ],
            compiler_params=pltpu.CompilerParams(collective_id=0, has_side_effects=True, vmem_limit_bytes=60 * 2**20),
            name="heads_attention",
        )(flat(queries), flat(keys), flat(values), flat(out_grad))
        shape = (batch, tokens, heads, dim)
        kv_shape = (batch, tokens, kv_heads, dim)
        row_lse = lse[:, :groups * ratio, :].reshape(batch, heads, tokens)
        return out.reshape(shape), row_lse, dq.reshape(shape), dk.reshape(kv_shape), dv.reshape(kv_shape)

    seq_spec = P("dp", "cp")
    return jax.shard_map(attention_shard, mesh=mesh, in_specs=(seq_spec,) * 4, out_specs=(seq_spec, P("dp", None, "cp"), seq_spec, seq_spec, seq_spec), check_vma=False)
```

```python
import functools

import jax
import jax.numpy as jnp
from jax import lax
from jax.experimental import pallas as pl
from jax.experimental.pallas import tpu as pltpu
from jax.sharding import PartitionSpec as P

MESH = pl.DeviceIdType.MESH
F32 = jnp.float32
BF16 = jnp.bfloat16
NT = (((1,), (1,)), ((), ()))


def attention_kernel(n, groups, ratio, tokens, dim, q_in, k_in, v_in, g_in, o_out, dq_out, dk_out, dv_out, lse_out, qb, kb, vb, gb, ob, dqb, dkb, dvb, lseb, s_scr, dk_acc, dv_acc, kt, vt, t_scr, q_cat, g_cat, q_stage, k_stage, v_stage, g_stage, q_send, k_send, v_send, g_send, f_scr, stage_sem, in_send, in_recv, out_send, out_recv, lse_send, lse_recv, in_local, out_local, lse_local):
    me = lax.axis_index("cp")
    scale = dim ** -0.5
    wide = ratio * dim

    def peer(offset):
        return {"cp": lax.rem(me + offset, n)}

    def row_of(device):
        return pl.ds(pl.multiple_of(device * tokens, tokens), tokens)

    def column_of(head, width):
        return pl.ds(pl.multiple_of(head * width, width), width)

    stages = ((k_in, k_stage), (v_in, v_stage), (q_in, q_stage), (g_in, g_stage))
    stage_copies = []
    for a, (src, dst) in enumerate(stages):
        copy = pltpu.make_async_copy(src, dst, stage_sem.at[a])
        copy.start()
        stage_copies.append(copy)

    barrier = pltpu.get_barrier_semaphore()
    for offset in range(1, n):
        pl.semaphore_signal(barrier, inc=1, device_id=peer(offset), device_id_type=MESH)

    def split_heads(stage, send):
        heads = stage.shape[1]
        per = heads // send.shape[0]
        pad = heads + 8
        step = 16

        def widen(t, _):
            base = t * step
            part = stage[pl.ds(base, step)].astype(F32)
            for u in range(step):
                f_scr[pl.ds(pl.multiple_of((base + u) * pad, 8), heads), :] = part[u]
            return 0

        lax.fori_loop(0, tokens // step, widen, 0)

        def gather(h, _):
            for r in range(per):
                send[h, :, r * dim:(r + 1) * dim] = f_scr[pl.ds(h * per + r, tokens, stride=pad), :].astype(BF16)
            return 0

        lax.fori_loop(0, send.shape[0], gather, 0)

    in_arrays = ((k_send, kb), (v_send, vb), (q_send, qb), (g_send, gb))
    in_copies = {}

    def send_in(g, a):
        src, dst = in_arrays[a]
        for offset in range(1, n):
            target = lax.rem(me + offset, n)
            copy = pltpu.make_async_remote_copy(
                src_ref=src.at[target * groups + g],
                dst_ref=dst.at[g, row_of(me)],
                send_sem=in_send.at[g, offset - 1, a],
                recv_sem=in_recv.at[g, offset - 1, a],
                device_id=peer(offset),
                device_id_type=MESH,
            )
            copy.start()
            in_copies[g, offset, a] = copy
        copy = pltpu.make_async_copy(src.at[me * groups + g], dst.at[g, row_of(me)], in_local.at[g, a])
        copy.start()
        in_copies[g, 0, a] = copy

    stage_copies[0].wait()
    split_heads(k_stage, k_send)
    stage_copies[1].wait()
    split_heads(v_stage, v_send)
    pl.semaphore_wait(barrier, n - 1)
    send_in(0, 0)
    stage_copies[2].wait()
    split_heads(q_stage, q_send)
    send_in(0, 1)
    stage_copies[3].wait()
    split_heads(g_stage, g_send)
    send_in(0, 2)
    send_in(0, 3)
    for g in range(1, groups):
        for a in range(4):
            send_in(g, a)

    blk = q_cat.shape[0] // ratio
    cols = ratio * blk
    key_pos = lax.broadcasted_iota(jnp.int32, (blk, blk), 0)
    query_pos = lax.broadcasted_iota(jnp.int32, (blk, blk), 1)

    def fold(x, op):
        return op(x.reshape(blk // 8, 8, cols), axis=0)

    def block_of(index):
        return pl.ds(pl.multiple_of(index * blk, blk), blk)

    def head_compute(g):
        def prepare(j, _):
            rows = block_of(j)
            kt[:, rows] = jnp.transpose(kb[g, rows, :].astype(F32)).astype(BF16)
            vt[:, rows] = jnp.transpose(vb[g, rows, :].astype(F32)).astype(BF16)
            dk_acc[rows, :] = jnp.zeros((blk, dim), F32)
            dv_acc[rows, :] = jnp.zeros((blk, dim), F32)
            return 0

        lax.fori_loop(0, n * tokens // blk, prepare, 0)

        def block(i, _):
            rows_i = block_of(i)
            for r in range(ratio):
                q_cat[r * blk:(r + 1) * blk, :] = qb[g, rows_i, r * dim:(r + 1) * dim]
                g_cat[r * blk:(r + 1) * blk, :] = gb[g, rows_i, r * dim:(r + 1) * dim]

            def score(j, top):
                rows = block_of(j)
                s = lax.dot_general(kb[g, rows, :], q_cat[...], NT, preferred_element_type=F32)
                s_scr[rows, :] = s
                return jnp.maximum(top, fold(s, jnp.max))

            top = lax.fori_loop(0, i, score, jnp.full((8, cols), -jnp.inf, F32))
            s = lax.dot_general(kb[g, rows_i, :], q_cat[...], NT, preferred_element_type=F32)
            keep = jnp.concatenate([key_pos <= query_pos] * ratio, axis=1)
            s = jnp.where(keep, s, -jnp.inf)
            s_scr[rows_i, :] = s
            top = jnp.max(jnp.maximum(top, fold(s, jnp.max)), axis=0, keepdims=True)

            def weigh(j, total):
                rows = block_of(j)
                p = jnp.exp((s_scr[rows, :] - top) * scale)
                s_scr[rows, :] = p
                return total + fold(p, jnp.sum)

            total = lax.fori_loop(0, i + 1, weigh, jnp.zeros((8, cols), F32))
            total = jnp.sum(total, axis=0, keepdims=True)
            inv = 1.0 / total
            lse = top * scale + jnp.log(total)
            for r in range(ratio):
                for t in range(blk // tokens):
                    at = r * blk + t * tokens
                    lseb[i * (blk // tokens) + t, pl.ds(g * ratio + r, 1), :] = lse[:, at:at + tokens]
            t_scr[...] = jnp.zeros((dim, cols), F32)

            def outputs(j, _):
                rows = block_of(j)
                p_low = (s_scr[rows, :] * inv).astype(BF16)
                t_scr[...] += jnp.dot(vt[:, rows], p_low, preferred_element_type=F32)
                dv_acc[rows, :] += jnp.dot(p_low, g_cat[...], preferred_element_type=F32)
                return 0

            lax.fori_loop(0, i + 1, outputs, 0)
            out = jnp.transpose(t_scr[...]).astype(BF16)
            for r in range(ratio):
                ob[g, rows_i, r * dim:(r + 1) * dim] = out[r * blk:(r + 1) * blk]
            delta = jnp.sum(jnp.transpose(g_cat[...].astype(F32) * out.astype(F32)), axis=0, keepdims=True)
            t_scr[...] = jnp.zeros((dim, cols), F32)

            def gradients(j, _):
                rows = block_of(j)
                dp = lax.dot_general(vb[g, rows, :], g_cat[...], NT, preferred_element_type=F32)
                ds = ((s_scr[rows, :] * inv) * (dp - delta)).astype(BF16)
                t_scr[...] += jnp.dot(kt[:, rows], ds, preferred_element_type=F32)
                dk_acc[rows, :] += jnp.dot(ds, q_cat[...], preferred_element_type=F32)
                return 0

            lax.fori_loop(0, i + 1, gradients, 0)
            dq = jnp.transpose(t_scr[...] * scale).astype(BF16)
            for r in range(ratio):
                dqb[g, rows_i, r * dim:(r + 1) * dim] = dq[r * blk:(r + 1) * blk]
            return 0

        lax.fori_loop(0, n * tokens // blk, block, 0)

        def finish(j, _):
            rows = block_of(j)
            dkb[g, rows, :] = (dk_acc[rows, :] * scale).astype(BF16)
            dvb[g, rows, :] = dv_acc[rows, :].astype(BF16)
            return 0

        lax.fori_loop(0, n * tokens // blk, finish, 0)

    out_arrays = ((ob, o_out, wide), (dqb, dq_out, wide), (dkb, dk_out, dim), (dvb, dv_out, dim))
    out_copies = {}
    for g in range(groups):
        for offset in range(n):
            for a in range(4):
                if offset:
                    in_copies[g, offset, a].wait_recv()
                else:
                    in_copies[g, offset, a].wait()
        head_compute(g)
        for offset in range(1, n):
            target = lax.rem(me + offset, n)
            for a, (src, dst, width) in enumerate(out_arrays):
                copy = pltpu.make_async_remote_copy(
                    src_ref=src.at[g, row_of(target)],
                    dst_ref=dst.at[:, column_of(me * groups + g, width)],
                    send_sem=out_send.at[g, offset - 1, a],
                    recv_sem=out_recv.at[g, offset - 1, a],
                    device_id=peer(offset),
                    device_id_type=MESH,
                )
                copy.start()
                out_copies[g, offset, a] = copy
        for a, (src, dst, width) in enumerate(out_arrays):
            copy = pltpu.make_async_copy(src.at[g, row_of(me)], dst.at[:, column_of(me * groups + g, width)], out_local.at[g, a])
            copy.start()
            out_copies[g, 0, a] = copy

    lse_copies = []
    for offset in range(1, n):
        target = lax.rem(me + offset, n)
        copy = pltpu.make_async_remote_copy(
            src_ref=lseb.at[target],
            dst_ref=lse_out.at[me],
            send_sem=lse_send.at[offset - 1],
            recv_sem=lse_recv.at[offset - 1],
            device_id=peer(offset),
            device_id_type=MESH,
        )
        copy.start()
        lse_copies.append(copy)
    copy = pltpu.make_async_copy(lseb.at[me], lse_out.at[me], lse_local)
    copy.start()
    lse_copies.append(copy)

    for (g, offset, a), copy in in_copies.items():
        if offset:
            copy.wait_send()
    for copy in out_copies.values():
        copy.wait()
    for copy in lse_copies:
        copy.wait()


def solution(mesh):
    n = mesh.shape["cp"]

    def attention_shard(queries, keys, values, out_grad):
        batch, tokens, heads, dim = queries.shape
        kv_heads = keys.shape[2]
        ratio = heads // kv_heads
        groups = kv_heads // n
        total = n * tokens
        wide = ratio * dim
        blk = 2 * tokens
        stats = -(-groups * ratio // 8) * 8

        def flat(x):
            return x.reshape(tokens, x.shape[2], dim)

        any_space = pl.BlockSpec(memory_space=pl.ANY)
        dma = pltpu.SemaphoreType.DMA
        out, dq, dk, dv, lse = pl.pallas_call(
            functools.partial(attention_kernel, n, groups, ratio, tokens, dim),
            out_shape=(
                jax.ShapeDtypeStruct((tokens, heads * dim), BF16),
                jax.ShapeDtypeStruct((tokens, heads * dim), BF16),
                jax.ShapeDtypeStruct((tokens, kv_heads * dim), BF16),
                jax.ShapeDtypeStruct((tokens, kv_heads * dim), BF16),
                jax.ShapeDtypeStruct((n, stats, tokens), F32),
            ),
            in_specs=[any_space] * 4,
            out_specs=(any_space,) * 5,
            scratch_shapes=[
                pltpu.VMEM((groups, total, wide), BF16),
                pltpu.VMEM((groups, total, dim), BF16),
                pltpu.VMEM((groups, total, dim), BF16),
                pltpu.VMEM((groups, total, wide), BF16),
                pltpu.VMEM((groups, total, wide), BF16),
                pltpu.VMEM((groups, total, wide), BF16),
                pltpu.VMEM((groups, total, dim), BF16),
                pltpu.VMEM((groups, total, dim), BF16),
                pltpu.VMEM((n, stats, tokens), F32),
                pltpu.VMEM((total, ratio * blk), F32),
                pltpu.VMEM((total, dim), F32),
                pltpu.VMEM((total, dim), F32),
                pltpu.VMEM((dim, total), BF16),
                pltpu.VMEM((dim, total), BF16),
                pltpu.VMEM((dim, ratio * blk), F32),
                pltpu.VMEM((ratio * blk, dim), BF16),
                pltpu.VMEM((ratio * blk, dim), BF16),
                pltpu.VMEM((tokens, heads, dim), BF16),
                pltpu.VMEM((tokens, kv_heads, dim), BF16),
                pltpu.VMEM((tokens, kv_heads, dim), BF16),
                pltpu.VMEM((tokens, heads, dim), BF16),
                pltpu.VMEM((kv_heads, tokens, wide), BF16),
                pltpu.VMEM((kv_heads, tokens, dim), BF16),
                pltpu.VMEM((kv_heads, tokens, dim), BF16),
                pltpu.VMEM((kv_heads, tokens, wide), BF16),
                pltpu.VMEM((tokens * (heads + 8), dim), F32),
                dma((4,)),
                dma((groups, n - 1, 4)),
                dma((groups, n - 1, 4)),
                dma((groups, n - 1, 4)),
                dma((groups, n - 1, 4)),
                dma((n - 1,)),
                dma((n - 1,)),
                dma((groups, 4)),
                dma((groups, 4)),
                dma,
            ],
            compiler_params=pltpu.CompilerParams(collective_id=0, has_side_effects=True, vmem_limit_bytes=60 * 2**20),
            name="heads_attention",
        )(flat(queries), flat(keys), flat(values), flat(out_grad))
        shape = (batch, tokens, heads, dim)
        kv_shape = (batch, tokens, kv_heads, dim)
        row_lse = lse[:, :groups * ratio, :].reshape(batch, heads, tokens)
        return out.reshape(shape), row_lse, dq.reshape(shape), dk.reshape(kv_shape), dv.reshape(kv_shape)

    seq_spec = P("dp", "cp")
    return jax.shard_map(attention_shard, mesh=mesh, in_specs=(seq_spec,) * 4, out_specs=(seq_spec, P("dp", None, "cp"), seq_spec, seq_spec, seq_spec), check_vma=False)
```

```python
import functools

import jax
import jax.numpy as jnp
from jax import lax
from jax.experimental import pallas as pl
from jax.experimental.pallas import tpu as pltpu
from jax.sharding import PartitionSpec as P

MESH = pl.DeviceIdType.MESH
F32 = jnp.float32
BF16 = jnp.bfloat16
NT = (((1,), (1,)), ((), ()))
CORES = 2
JOB_CHIPS = 2


def attention_kernel(n, groups, ratio, tokens, dim, q_in, k_in, v_in, g_in, o_out, dq_out, dk_out, dv_out, lse_out, qb, kb, vb, gb, ob, dqb, dkb, dvb, lseb, s_scr, dk_acc, dv_acc, kt, vt, t_scr, q_cat, g_cat, q_stage, k_stage, v_stage, g_stage, q_send, k_send, v_send, g_send, f_scr, jq, jk, jv, jg, jl, j_own, j_part, j_recv, o_part, stage_sem, in_send, in_recv, out_send, out_recv, lse_send, lse_recv, in_local, out_local, lse_local, ji_send, ji_recv, ji_local, jk_send, jk_recv, jo_send, jo_recv, jo_local, jl_send, jl_recv, jl_local, o_part_send, j_part_send, part_recv, fin_send, fin_recv, fin_local):
    me = lax.axis_index("cp")
    chip = lax.div(me, CORES)
    core = lax.rem(me, CORES)
    chips = n // CORES
    scale = dim ** -0.5
    wide = ratio * dim
    blk = CORES * tokens
    cols = ratio * blk
    rows_total = chips * blk
    slots = (chips - 1) * groups
    jobs = jnp.where(chip == 0, slots, jnp.where(chip == 1, groups, 0))

    def first_row(owner_chip):
        return lax.div(owner_chip + 1, 2)

    def peer(offset):
        return {"cp": lax.rem(me + offset, n)}

    partner = {"cp": me + 1 - 2 * core}

    def row_of(device):
        return pl.ds(pl.multiple_of(device * tokens, tokens), tokens)

    def block_of(index):
        return pl.ds(pl.multiple_of(index * blk, blk), blk)

    def column_of(head, width):
        return pl.ds(pl.multiple_of(head * width, width), width)

    def remote(src, dst, send_sem, recv_sem, device):
        return pltpu.make_async_remote_copy(src_ref=src, dst_ref=dst, send_sem=send_sem, recv_sem=recv_sem, device_id=device, device_id_type=MESH)

    pending = []

    def launch(copy, sends=None, receives=None):
        if sends is None:
            copy.start()
        else:
            pl.when(sends)(copy.start)
        pending.append((copy.wait_send, sends))
        return (copy, receives)

    def landed(entry):
        copy, receives = entry
        if receives is None:
            copy.wait_recv()
        else:
            pl.when(receives)(copy.wait_recv)

    def local(src, dst, sem, cond=None):
        copy = pltpu.make_async_copy(src, dst, sem)
        if cond is None:
            copy.start()
        else:
            pl.when(cond)(copy.start)
        return (copy, cond)

    def done(entry):
        copy, cond = entry
        if cond is None:
            copy.wait()
        else:
            pl.when(cond)(copy.wait)

    stage_copies = [local(src, dst, stage_sem.at[a]) for a, (src, dst) in enumerate(((k_in, k_stage), (v_in, v_stage), (q_in, q_stage), (g_in, g_stage)))]

    barrier = pltpu.get_barrier_semaphore()
    for offset in range(1, n):
        pl.semaphore_signal(barrier, inc=1, device_id=peer(offset), device_id_type=MESH)

    def split_heads(stage, send):
        heads = stage.shape[1]
        per = heads // send.shape[0]
        pad = heads + 8
        step = 16
        half = tokens // 2
        for part in range(2):
            def widen(t, _):
                base = t * step
                piece = stage[pl.ds(part * half + base, step)].astype(F32)
                for u in range(step):
                    f_scr[pl.ds(pl.multiple_of((base + u) * pad, 8), heads), :] = piece[u]
                return 0

            lax.fori_loop(0, half // step, widen, 0)

            def gather(h, _):
                for r in range(per):
                    send[h, part * half:(part + 1) * half, r * dim:(r + 1) * dim] = f_scr[pl.ds(h * per + r, half, stride=pad), :].astype(BF16)
                return 0

            lax.fori_loop(0, send.shape[0], gather, 0)

    in_arrays = ((k_send, kb), (v_send, vb), (q_send, qb), (g_send, gb))
    job_arrays = ((k_send, jk), (v_send, jv), (q_send, jq), (g_send, jg))
    arrived = {}
    job_arrived = []

    def send_in(g, a):
        src, dst = in_arrays[a]
        for offset in range(1, n):
            target = lax.rem(me + offset, n)
            sends = receives = None
            if a >= 2:
                sends = chip >= first_row(lax.div(target, CORES))
                receives = lax.div(lax.rem(me + n - offset, n), CORES) >= first_row(chip)
            copy = remote(src.at[target * groups + g], dst.at[g, row_of(me)], in_send.at[g, offset - 1, a], in_recv.at[g, offset - 1, a], peer(offset))
            arrived[g, offset, a] = launch(copy, sends, receives)
        arrived[g, 0, a] = local(src.at[me * groups + g], dst.at[g, row_of(me)], in_local.at[g, a])

    def job_head(slot, which_core):
        owner_chip = jnp.where(chip == 0, 1 + slot // groups, chips - 1)
        return (CORES * owner_chip + which_core) * groups + slot % groups

    def job_rows(slot):
        return (slot * (chip + 1) + chip) * blk

    def tokens_at(base, which_core):
        return pl.ds(pl.multiple_of(base + which_core * tokens, tokens), tokens)

    def send_job(a):
        src, dst = job_arrays[a]
        for s in range(slots):
            base = job_rows(s) if a < 2 else s * blk
            place = dst.at[tokens_at(base, core)]
            copy = remote(src.at[job_head(s, 1 - core)], place, ji_send.at[s, a], ji_recv.at[s, a], partner)
            job_arrived.append((landed, launch(copy, s < jobs, s < jobs)))
            job_arrived.append((done, local(src.at[job_head(s, core)], place, ji_local.at[s, a], s < jobs)))

    done(stage_copies[0])
    split_heads(k_stage, k_send)
    done(stage_copies[1])
    split_heads(v_stage, v_send)
    pl.semaphore_wait(barrier, n - 1)
    send_job(0)
    for k in range(CORES):
        for g in range(groups):
            for a in range(2):
                src, dst = job_arrays[a]
                copy = remote(
                    src.at[(CORES * (chips - 1) + k) * groups + g],
                    dst.at[tokens_at(g * 2 * blk, core)],
                    jk_send.at[k, g, a],
                    jk_recv.at[core, g, a],
                    {"cp": CORES + k},
                )
                launch(copy, chip == 0)
    send_in(0, 0)
    done(stage_copies[2])
    split_heads(q_stage, q_send)
    send_job(1)
    send_job(2)
    send_in(0, 1)
    done(stage_copies[3])
    split_heads(g_stage, g_send)
    send_in(0, 2)
    send_job(3)
    send_in(0, 3)
    for g in range(1, groups):
        for a in range(4):
            send_in(g, a)

    key_pos = lax.broadcasted_iota(jnp.int32, (blk, blk), 0)
    query_pos = lax.broadcasted_iota(jnp.int32, (blk, blk), 1)

    def fold(x, op):
        return op(x.reshape(blk // 8, 8, cols), axis=0)

    def prepare(j, key, value):
        rows = block_of(j)
        kt[:, rows] = jnp.transpose(key(j).astype(F32)).astype(BF16)
        vt[:, rows] = jnp.transpose(value(j).astype(F32)).astype(BF16)
        dk_acc[rows, :] = jnp.zeros((blk, dim), F32)
        dv_acc[rows, :] = jnp.zeros((blk, dim), F32)

    def block(i, key, value, query, cotangent, put_lse, put_out, put_dq):
        rows_i = block_of(i)
        for r in range(ratio):
            q_cat[r * blk:(r + 1) * blk, :] = query(r)
            g_cat[r * blk:(r + 1) * blk, :] = cotangent(r)

        def score(j, top):
            s = lax.dot_general(key(j), q_cat[...], NT, preferred_element_type=F32)
            s_scr[block_of(j), :] = s
            return jnp.maximum(top, fold(s, jnp.max))

        top = lax.fori_loop(0, i, score, jnp.full((8, cols), -jnp.inf, F32))
        s = lax.dot_general(key(i), q_cat[...], NT, preferred_element_type=F32)
        keep = jnp.concatenate([key_pos <= query_pos] * ratio, axis=1)
        s = jnp.where(keep, s, -jnp.inf)
        s_scr[rows_i, :] = s
        top = jnp.max(jnp.maximum(top, fold(s, jnp.max)), axis=0, keepdims=True)

        def weigh(j, total):
            rows = block_of(j)
            p = jnp.exp((s_scr[rows, :] - top) * scale)
            s_scr[rows, :] = p
            return total + fold(p, jnp.sum)

        total = lax.fori_loop(0, i + 1, weigh, jnp.zeros((8, cols), F32))
        total = jnp.sum(total, axis=0, keepdims=True)
        inv = 1.0 / total
        lse = top * scale + jnp.log(total)
        for r in range(ratio):
            for t in range(CORES):
                at = r * blk + t * tokens
                put_lse(r, t, lse[:, at:at + tokens])
        t_scr[...] = jnp.zeros((dim, cols), F32)

        def outputs(j, _):
            rows = block_of(j)
            p_low = (s_scr[rows, :] * inv).astype(BF16)
            t_scr[...] += jnp.dot(vt[:, rows], p_low, preferred_element_type=F32)
            dv_acc[rows, :] += jnp.dot(p_low, g_cat[...], preferred_element_type=F32)
            return 0

        lax.fori_loop(0, i + 1, outputs, 0)
        out = jnp.transpose(t_scr[...]).astype(BF16)
        for r in range(ratio):
            put_out(r, out[r * blk:(r + 1) * blk])
        delta = jnp.sum(jnp.transpose(g_cat[...].astype(F32) * out.astype(F32)), axis=0, keepdims=True)
        t_scr[...] = jnp.zeros((dim, cols), F32)

        def gradients(j, _):
            rows = block_of(j)
            dp = lax.dot_general(value(j), g_cat[...], NT, preferred_element_type=F32)
            ds = ((s_scr[rows, :] * inv) * (dp - delta)).astype(BF16)
            t_scr[...] += jnp.dot(kt[:, rows], ds, preferred_element_type=F32)
            dk_acc[rows, :] += jnp.dot(ds, q_cat[...], preferred_element_type=F32)
            return 0

        lax.fori_loop(0, i + 1, gradients, 0)
        dq = jnp.transpose(t_scr[...] * scale).astype(BF16)
        for r in range(ratio):
            put_dq(r, dq[r * blk:(r + 1) * blk])

    for wait, entry in job_arrived:
        wait(entry)
    for j in range(CORES):
        for g in range(groups):
            for a in range(2):
                src, dst = job_arrays[a]
                copy = remote(src.at[0], dst.at[tokens_at(g * 2 * blk, j)], jk_send.at[0, g, a], jk_recv.at[j, g, a], partner)
                landed((copy, chip == 1))

    def job(s, _):
        def key(j):
            return jk[pl.ds(pl.multiple_of((s * (chip + 1) + j) * blk, blk), blk), :]

        def value(j):
            return jv[pl.ds(pl.multiple_of((s * (chip + 1) + j) * blk, blk), blk), :]

        def lanes(r):
            return slice(r * dim, (r + 1) * dim)

        rows = block_of(s)
        group = lax.div(s, groups)
        stat = lax.rem(s, groups) * ratio

        def put_lse(r, t, x):
            jl[group, t, pl.ds(stat + r, 1), :] = x

        def put_out(r, x):
            jq[rows, lanes(r)] = x

        def put_dq(r, x):
            jg[rows, lanes(r)] = x

        def prep(j, _):
            prepare(j, key, value)
            return 0

        lax.fori_loop(0, chip + 1, prep, 0)
        block(chip, key, value, lambda r: jq[rows, lanes(r)], lambda r: jg[rows, lanes(r)], put_lse, put_out, put_dq)
        own = block_of(chip)
        j_own[s, 0] = dk_acc[own, :] * scale
        j_own[s, 1] = dv_acc[own, :]

        @pl.when(chip == 1)
        def _():
            j_part[s, 0] = dk_acc[0:blk, :] * scale
            j_part[s, 1] = dv_acc[0:blk, :]

        return 0

    lax.fori_loop(0, jobs, job, 0)

    closing = []
    for g in range(groups):
        copy = remote(j_part.at[g], j_recv.at[slots + g], j_part_send.at[g], part_recv.at[slots + g], {"cp": core})
        launch(copy, chip == 1)
    for s in range(slots):
        for a, (src, dst) in enumerate(((jq, o_out), (jg, dq_out))):
            place = dst.at[:, column_of(job_head(s, core), wide)]
            copy = remote(src.at[tokens_at(s * blk, 1 - core)], place, jo_send.at[s, a], jo_recv.at[s, a], partner)
            closing.append((landed, launch(copy, s < jobs, s < jobs)))
            closing.append((done, local(src.at[tokens_at(s * blk, core)], place, jo_local.at[s, a], s < jobs)))
    for c in range(chips - 1):
        busy = c * groups < jobs
        owner = CORES * jnp.where(chip == 0, 1 + c, chips - 1) + core
        copy = remote(jl.at[c, 1 - core], lse_out.at[owner], jl_send.at[c], jl_recv.at[c], partner)
        closing.append((landed, launch(copy, busy, busy)))
        closing.append((done, local(jl.at[c, core], lse_out.at[owner], jl_local.at[c], busy)))

    def head_compute(g):
        def key(j):
            return kb[g, block_of(j), :]

        def value(j):
            return vb[g, block_of(j), :]

        def lanes(r):
            return slice(r * dim, (r + 1) * dim)

        def prep(j, _):
            prepare(j, key, value)
            return 0

        lax.fori_loop(0, chips, prep, 0)

        def row(i, _):
            rows = block_of(i)

            def put_lse(r, t, x):
                lseb[i * CORES + t, pl.ds(g * ratio + r, 1), :] = x

            def put_out(r, x):
                ob[g, rows, lanes(r)] = x

            def put_dq(r, x):
                dqb[g, rows, lanes(r)] = x

            block(i, key, value, lambda r: qb[g, rows, lanes(r)], lambda r: gb[g, rows, lanes(r)], put_lse, put_out, put_dq)
            return 0

        lax.fori_loop(first_row(chip), chips, row, 0)

        def finish(j, _):
            rows = block_of(j)
            dkb[g, rows, :] = (dk_acc[rows, :] * scale).astype(BF16)
            dvb[g, rows, :] = dv_acc[rows, :].astype(BF16)
            return 0

        lax.fori_loop(first_row(chip), chips, finish, 0)
        for b in range(JOB_CHIPS):
            @pl.when(b < first_row(chip))
            def _():
                o_part[g, b, 0] = dk_acc[b * blk:(b + 1) * blk, :] * scale
                o_part[g, b, 1] = dv_acc[b * blk:(b + 1) * blk, :]

    out_arrays = ((ob, o_out, wide), (dqb, dq_out, wide), (dkb, dk_out, dim), (dvb, dv_out, dim))
    for g in range(groups):
        for offset in range(n):
            for a in range(4):
                (landed if offset else done)(arrived[g, offset, a])
        head_compute(g)
        for b in range(JOB_CHIPS):
            slot = (chip - 1) * groups + g if b == 0 else g
            sends = b < first_row(chip)
            slot = jnp.where(sends, slot, 0)
            copy = remote(o_part.at[g, b], j_recv.at[slot], o_part_send.at[g, b], part_recv.at[slot], {"cp": CORES * b + core})
            launch(copy, sends)
        for offset in range(1, n):
            target = lax.rem(me + offset, n)
            sends = lax.div(target, CORES) >= first_row(chip)
            receives = chip >= first_row(lax.div(lax.rem(me + n - offset, n), CORES))
            for a, (src, dst, width) in enumerate(out_arrays):
                copy = remote(src.at[g, row_of(target)], dst.at[:, column_of(me * groups + g, width)], out_send.at[g, offset - 1, a], out_recv.at[g, offset - 1, a], peer(offset))
                closing.append((landed, launch(copy, sends, receives)))
        for a, (src, dst, width) in enumerate(out_arrays):
            closing.append((done, local(src.at[g, row_of(me)], dst.at[:, column_of(me * groups + g, width)], out_local.at[g, a])))

    for offset in range(1, n):
        target = lax.rem(me + offset, n)
        sends = lax.div(target, CORES) >= first_row(chip)
        receives = chip >= first_row(lax.div(lax.rem(me + n - offset, n), CORES))
        copy = remote(lseb.at[target], lse_out.at[me], lse_send.at[offset - 1], lse_recv.at[offset - 1], peer(offset))
        closing.append((landed, launch(copy, sends, receives)))
    closing.append((done, local(lseb.at[me], lse_out.at[me], lse_local)))

    for s in range(slots + groups):
        wanted = (chip == 0) | ((chip == 1) & (s < groups)) if s < groups else chip == 0
        copy = remote(j_part.at[0], j_recv.at[s], j_part_send.at[0], part_recv.at[s], partner)
        landed((copy, wanted))

    def total_of(s, _):
        last = jnp.where(chip == 0, s - (chips - 2) * groups, -1)
        rows = pl.ds(pl.multiple_of((s * (chip + 1) + chip) * blk, blk), blk)
        for a, dst in enumerate((jk, jv)):
            j_own[s, a] += j_recv[s, a]

            @pl.when(last >= 0)
            def _():
                j_own[s, a] += j_recv[slots + last, a]

            dst[rows, :] = j_own[s, a].astype(BF16)
        return 0

    lax.fori_loop(0, jobs, total_of, 0)
    for s in range(slots):
        for a, (src, dst) in enumerate(((jk, dk_out), (jv, dv_out))):
            place = dst.at[:, column_of(job_head(s, core), dim)]
            base = job_rows(s)
            copy = remote(src.at[tokens_at(base, 1 - core)], place, fin_send.at[s, a], fin_recv.at[s, a], partner)
            closing.append((landed, launch(copy, s < jobs, s < jobs)))
            closing.append((done, local(src.at[tokens_at(base, core)], place, fin_local.at[s, a], s < jobs)))

    for wait, entry in closing:
        wait(entry)
    for wait, cond in pending:
        if cond is None:
            wait()
        else:
            pl.when(cond)(wait)


def solution(mesh):
    n = mesh.shape["cp"]

    def attention_shard(queries, keys, values, out_grad):
        batch, tokens, heads, dim = queries.shape
        kv_heads = keys.shape[2]
        ratio = heads // kv_heads
        groups = kv_heads // n
        total = n * tokens
        wide = ratio * dim
        blk = CORES * tokens
        slots = (n // CORES - 1) * groups
        stats = -(-groups * ratio // 8) * 8

        def flat(x):
            return x.reshape(tokens, x.shape[2], dim)

        any_space = pl.BlockSpec(memory_space=pl.ANY)
        vmem = pltpu.VMEM
        dma = pltpu.SemaphoreType.DMA
        out, dq, dk, dv, lse = pl.pallas_call(
            functools.partial(attention_kernel, n, groups, ratio, tokens, dim),
            out_shape=(
                jax.ShapeDtypeStruct((tokens, heads * dim), BF16),
                jax.ShapeDtypeStruct((tokens, heads * dim), BF16),
                jax.ShapeDtypeStruct((tokens, kv_heads * dim), BF16),
                jax.ShapeDtypeStruct((tokens, kv_heads * dim), BF16),
                jax.ShapeDtypeStruct((n, stats, tokens), F32),
            ),
            in_specs=[any_space] * 4,
            out_specs=(any_space,) * 5,
            scratch_shapes=[
                vmem((groups, total, wide), BF16),
                vmem((groups, total, dim), BF16),
                vmem((groups, total, dim), BF16),
                vmem((groups, total, wide), BF16),
                vmem((groups, total, wide), BF16),
                vmem((groups, total, wide), BF16),
                vmem((groups, total, dim), BF16),
                vmem((groups, total, dim), BF16),
                vmem((n, stats, tokens), F32),
                vmem((total, ratio * blk), F32),
                vmem((total, dim), F32),
                vmem((total, dim), F32),
                vmem((dim, total), BF16),
                vmem((dim, total), BF16),
                vmem((dim, ratio * blk), F32),
                vmem((ratio * blk, dim), BF16),
                vmem((ratio * blk, dim), BF16),
                vmem((tokens, heads, dim), BF16),
                vmem((tokens, kv_heads, dim), BF16),
                vmem((tokens, kv_heads, dim), BF16),
                vmem((tokens, heads, dim), BF16),
                vmem((kv_heads, tokens, wide), BF16),
                vmem((kv_heads, tokens, dim), BF16),
                vmem((kv_heads, tokens, dim), BF16),
                vmem((kv_heads, tokens, wide), BF16),
                vmem((tokens // 2 * (heads + 8), dim), F32),
                vmem((slots * blk, wide), BF16),
                vmem((slots * blk, dim), BF16),
                vmem((slots * blk, dim), BF16),
                vmem((slots * blk, wide), BF16),
                vmem((n // CORES - 1, CORES, stats, tokens), F32),
                vmem((slots, 2, blk, dim), F32),
                vmem((groups, 2, blk, dim), F32),
                vmem((slots + groups, 2, blk, dim), F32),
                vmem((groups, JOB_CHIPS, 2, blk, dim), F32),
                dma((4,)),
                dma((groups, n - 1, 4)),
                dma((groups, n - 1, 4)),
                dma((groups, n - 1, 4)),
                dma((groups, n - 1, 4)),
                dma((n - 1,)),
                dma((n - 1,)),
                dma((groups, 4)),
                dma((groups, 4)),
                dma,
                dma((slots, 4)),
                dma((slots, 4)),
                dma((slots, 4)),
                dma((CORES, groups, 2)),
                dma((CORES, groups, 2)),
                dma((slots, 2)),
                dma((slots, 2)),
                dma((slots, 2)),
                dma((n // CORES - 1,)),
                dma((n // CORES - 1,)),
                dma((n // CORES - 1,)),
                dma((groups, JOB_CHIPS)),
                dma((groups,)),
                dma((slots + groups,)),
                dma((slots, 2)),
                dma((slots, 2)),
                dma((slots, 2)),
            ],
            compiler_params=pltpu.CompilerParams(collective_id=0, has_side_effects=True, vmem_limit_bytes=62 * 2**20),
            name="heads_attention",
        )(flat(queries), flat(keys), flat(values), flat(out_grad))
        shape = (batch, tokens, heads, dim)
        kv_shape = (batch, tokens, kv_heads, dim)
        row_lse = lse[:, :groups * ratio, :].reshape(batch, heads, tokens)
        return out.reshape(shape), row_lse, dq.reshape(shape), dk.reshape(kv_shape), dv.reshape(kv_shape)

    seq_spec = P("dp", "cp")
    return jax.shard_map(attention_shard, mesh=mesh, in_specs=(seq_spec,) * 4, out_specs=(seq_spec, P("dp", None, "cp"), seq_spec, seq_spec, seq_spec), check_vma=False)
```

```python
import functools

import jax
import jax.numpy as jnp
from jax import lax
from jax.experimental import pallas as pl
from jax.experimental.pallas import tpu as pltpu
from jax.sharding import PartitionSpec as P

MESH = pl.DeviceIdType.MESH
F32 = jnp.float32
BF16 = jnp.bfloat16
NT = (((1,), (1,)), ((), ()))
CORES = 2
JOB_CHIPS = 2


def attention_kernel(n, groups, ratio, tokens, dim, q_in, k_in, v_in, g_in, o_out, dq_out, dk_out, dv_out, lse_out, qb, kb, vb, gb, ob, dqb, dkb, dvb, lseb, s_scr, dk_acc, dv_acc, kt, vt, t_scr, q_cat, g_cat, q_stage, k_stage, v_stage, g_stage, q_send, k_send, v_send, g_send, f_scr, jq, jk, jv, jg, jl, j_own, j_part, j_recv, o_part, stage_sem, in_send, in_recv, out_send, out_recv, lse_send, lse_recv, in_local, out_local, lse_local, ji_send, ji_recv, ji_local, jk_send, jk_recv, jo_send, jo_recv, jo_local, jl_send, jl_recv, jl_local, o_part_send, j_part_send, part_recv, fin_send, fin_recv, fin_local):
    me = lax.axis_index("cp")
    chip = lax.div(me, CORES)
    core = lax.rem(me, CORES)
    chips = n // CORES
    scale = dim ** -0.5
    wide = ratio * dim
    blk = CORES * tokens
    cols = ratio * blk
    rows_total = chips * blk
    slots = (chips - 1) * groups
    jobs = jnp.where(chip == 0, slots, jnp.where(chip == 1, groups, 0))

    def first_row(owner_chip):
        return lax.div(owner_chip + 1, 2)

    def peer(offset):
        return {"cp": lax.rem(me + offset, n)}

    partner = {"cp": me + 1 - 2 * core}

    def row_of(device):
        return pl.ds(pl.multiple_of(device * tokens, tokens), tokens)

    def block_of(index):
        return pl.ds(pl.multiple_of(index * blk, blk), blk)

    def column_of(head, width):
        return pl.ds(pl.multiple_of(head * width, width), width)

    def remote(src, dst, send_sem, recv_sem, device):
        return pltpu.make_async_remote_copy(src_ref=src, dst_ref=dst, send_sem=send_sem, recv_sem=recv_sem, device_id=device, device_id_type=MESH)

    pending = []

    def launch(copy, sends=None, receives=None):
        if sends is None:
            copy.start()
        else:
            pl.when(sends)(copy.start)
        pending.append((send_done, (copy, sends)))
        return (copy, receives)

    def landed(entry):
        copy, receives = entry
        if receives is None:
            copy.wait_recv()
        else:
            pl.when(receives)(copy.wait_recv)

    def send_done(entry):
        copy, sends = entry
        if sends is None:
            copy.wait_send()
        else:
            pl.when(sends)(copy.wait_send)

    def local(src, dst, sem, cond=None):
        copy = pltpu.make_async_copy(src, dst, sem)
        if cond is None:
            copy.start()
        else:
            pl.when(cond)(copy.start)
        return (copy, cond)

    def done(entry):
        copy, cond = entry
        if cond is None:
            copy.wait()
        else:
            pl.when(cond)(copy.wait)

    stage_copies = [local(src, dst, stage_sem.at[a]) for a, (src, dst) in enumerate(((k_in, k_stage), (v_in, v_stage), (q_in, q_stage), (g_in, g_stage)))]

    barrier = pltpu.get_barrier_semaphore()
    for offset in range(1, n):
        pl.semaphore_signal(barrier, inc=1, device_id=peer(offset), device_id_type=MESH)

    def split_heads(stage, send):
        heads = stage.shape[1]
        per = heads // send.shape[0]
        pad = heads + 8
        step = 16
        half = tokens // 2
        for part in range(2):
            def widen(t, _):
                base = t * step
                piece = stage[pl.ds(part * half + base, step)].astype(F32)
                for u in range(step):
                    f_scr[pl.ds(pl.multiple_of((base + u) * pad, 8), heads), :] = piece[u]
                return 0

            lax.fori_loop(0, half // step, widen, 0)

            def gather(h, _):
                for r in range(per):
                    send[h, part * half:(part + 1) * half, r * dim:(r + 1) * dim] = f_scr[pl.ds(h * per + r, half, stride=pad), :].astype(BF16)
                return 0

            lax.fori_loop(0, send.shape[0], gather, 0)

    in_arrays = ((k_send, kb), (v_send, vb), (q_send, qb), (g_send, gb))
    job_arrays = ((k_send, jk), (v_send, jv), (q_send, jq), (g_send, jg))
    arrived = {}
    job_arrived = []

    def send_in(g, a):
        src, dst = in_arrays[a]
        for offset in range(1, n):
            target = lax.rem(me + offset, n)
            sends = receives = None
            if a >= 2:
                sends = chip >= first_row(lax.div(target, CORES))
                receives = lax.div(lax.rem(me + n - offset, n), CORES) >= first_row(chip)
            copy = remote(src.at[target * groups + g], dst.at[g, row_of(me)], in_send.at[g, offset - 1, a], in_recv.at[g, offset - 1, a], peer(offset))
            arrived[g, offset, a] = launch(copy, sends, receives)
        arrived[g, 0, a] = local(src.at[me * groups + g], dst.at[g, row_of(me)], in_local.at[g, a])

    def job_head(slot, which_core):
        owner_chip = jnp.where(chip == 0, 1 + slot // groups, chips - 1)
        return (CORES * owner_chip + which_core) * groups + slot % groups

    def job_rows(slot):
        return (slot * (chip + 1) + chip) * blk

    def tokens_at(base, which_core):
        return pl.ds(pl.multiple_of(base + which_core * tokens, tokens), tokens)

    def send_job(a):
        src, dst = job_arrays[a]
        for s in range(slots):
            base = job_rows(s) if a < 2 else s * blk
            place = dst.at[tokens_at(base, core)]
            copy = remote(src.at[job_head(s, 1 - core)], place, ji_send.at[s, a], ji_recv.at[s, a], partner)
            job_arrived.append((landed, launch(copy, s < jobs, s < jobs)))
            job_arrived.append((done, local(src.at[job_head(s, core)], place, ji_local.at[s, a], s < jobs)))

    done(stage_copies[0])
    split_heads(k_stage, k_send)
    done(stage_copies[1])
    pl.semaphore_wait(barrier, n - 1)
    send_in(0, 0)
    split_heads(v_stage, v_send)
    send_job(0)
    for k in range(CORES):
        for g in range(groups):
            for a in range(2):
                src, dst = job_arrays[a]
                copy = remote(
                    src.at[(CORES * (chips - 1) + k) * groups + g],
                    dst.at[tokens_at(g * 2 * blk, core)],
                    jk_send.at[k, g, a],
                    jk_recv.at[core, g, a],
                    {"cp": CORES + k},
                )
                launch(copy, chip == 0)
    done(stage_copies[2])
    split_heads(q_stage, q_send)
    send_job(1)
    send_job(2)
    send_in(0, 1)
    done(stage_copies[3])
    split_heads(g_stage, g_send)
    send_in(0, 2)
    send_job(3)
    send_in(0, 3)
    for g in range(1, groups):
        for a in range(4):
            send_in(g, a)

    key_pos = lax.broadcasted_iota(jnp.int32, (blk, blk), 0)
    query_pos = lax.broadcasted_iota(jnp.int32, (blk, blk), 1)

    def fold(x, op):
        return op(x.reshape(blk // 8, 8, cols), axis=0)

    def prepare(j, key, value):
        rows = block_of(j)
        kt[:, rows] = jnp.transpose(key(j).astype(F32)).astype(BF16)
        vt[:, rows] = jnp.transpose(value(j).astype(F32)).astype(BF16)
        dk_acc[rows, :] = jnp.zeros((blk, dim), F32)
        dv_acc[rows, :] = jnp.zeros((blk, dim), F32)

    def block(i, key, value, query, cotangent, put_lse, put_out, put_dq):
        rows_i = block_of(i)
        for r in range(ratio):
            q_cat[r * blk:(r + 1) * blk, :] = query(r)
            g_cat[r * blk:(r + 1) * blk, :] = cotangent(r)

        def score(j, top):
            s = lax.dot_general(key(j), q_cat[...], NT, preferred_element_type=F32)
            s_scr[block_of(j), :] = s
            return jnp.maximum(top, fold(s, jnp.max))

        top = lax.fori_loop(0, i, score, jnp.full((8, cols), -jnp.inf, F32))
        s = lax.dot_general(key(i), q_cat[...], NT, preferred_element_type=F32)
        keep = jnp.concatenate([key_pos <= query_pos] * ratio, axis=1)
        s = jnp.where(keep, s, -jnp.inf)
        s_scr[rows_i, :] = s
        top = jnp.max(jnp.maximum(top, fold(s, jnp.max)), axis=0, keepdims=True)

        def weigh(j, total):
            rows = block_of(j)
            p = jnp.exp((s_scr[rows, :] - top) * scale)
            s_scr[rows, :] = p
            return total + fold(p, jnp.sum)

        total = lax.fori_loop(0, i + 1, weigh, jnp.zeros((8, cols), F32))
        total = jnp.sum(total, axis=0, keepdims=True)
        inv = 1.0 / total
        lse = top * scale + jnp.log(total)
        for r in range(ratio):
            for t in range(CORES):
                at = r * blk + t * tokens
                put_lse(r, t, lse[:, at:at + tokens])
        t_scr[...] = jnp.zeros((dim, cols), F32)

        def outputs(j, _):
            rows = block_of(j)
            p_low = (s_scr[rows, :] * inv).astype(BF16)
            t_scr[...] += jnp.dot(vt[:, rows], p_low, preferred_element_type=F32)
            dv_acc[rows, :] += jnp.dot(p_low, g_cat[...], preferred_element_type=F32)
            return 0

        lax.fori_loop(0, i + 1, outputs, 0)
        out = jnp.transpose(t_scr[...]).astype(BF16)
        for r in range(ratio):
            put_out(r, out[r * blk:(r + 1) * blk])
        delta = jnp.sum(jnp.transpose(g_cat[...].astype(F32) * out.astype(F32)), axis=0, keepdims=True)
        t_scr[...] = jnp.zeros((dim, cols), F32)

        def gradients(j, _):
            rows = block_of(j)
            dp = lax.dot_general(value(j), g_cat[...], NT, preferred_element_type=F32)
            ds = ((s_scr[rows, :] * inv) * (dp - delta)).astype(BF16)
            t_scr[...] += jnp.dot(kt[:, rows], ds, preferred_element_type=F32)
            dk_acc[rows, :] += jnp.dot(ds, q_cat[...], preferred_element_type=F32)
            return 0

        lax.fori_loop(0, i + 1, gradients, 0)
        dq = jnp.transpose(t_scr[...] * scale).astype(BF16)
        for r in range(ratio):
            put_dq(r, dq[r * blk:(r + 1) * blk])

    for wait, entry in job_arrived:
        wait(entry)
    for j in range(CORES):
        for g in range(groups):
            for a in range(2):
                src, dst = job_arrays[a]
                copy = remote(src.at[0], dst.at[tokens_at(g * 2 * blk, j)], jk_send.at[0, g, a], jk_recv.at[j, g, a], partner)
                landed((copy, chip == 1))

    def job(s, _):
        def key(j):
            return jk[pl.ds(pl.multiple_of((s * (chip + 1) + j) * blk, blk), blk), :]

        def value(j):
            return jv[pl.ds(pl.multiple_of((s * (chip + 1) + j) * blk, blk), blk), :]

        def lanes(r):
            return slice(r * dim, (r + 1) * dim)

        rows = block_of(s)
        group = lax.div(s, groups)
        stat = lax.rem(s, groups) * ratio

        def put_lse(r, t, x):
            jl[group, t, pl.ds(stat + r, 1), :] = x

        def put_out(r, x):
            jq[rows, lanes(r)] = x

        def put_dq(r, x):
            jg[rows, lanes(r)] = x

        def prep(j, _):
            prepare(j, key, value)
            return 0

        lax.fori_loop(0, chip + 1, prep, 0)
        block(chip, key, value, lambda r: jq[rows, lanes(r)], lambda r: jg[rows, lanes(r)], put_lse, put_out, put_dq)
        own = block_of(chip)
        j_own[s, 0] = dk_acc[own, :] * scale
        j_own[s, 1] = dv_acc[own, :]

        @pl.when(chip == 1)
        def _():
            j_part[s, 0] = dk_acc[0:blk, :] * scale
            j_part[s, 1] = dv_acc[0:blk, :]

        return 0

    lax.fori_loop(0, jobs, job, 0)

    closing = []
    for g in range(groups):
        copy = remote(j_part.at[g], j_recv.at[slots + g], j_part_send.at[g], part_recv.at[slots + g], {"cp": core})
        launch(copy, chip == 1)
    for s in range(slots):
        for a, (src, dst) in enumerate(((jq, o_out), (jg, dq_out))):
            place = dst.at[:, column_of(job_head(s, core), wide)]
            copy = remote(src.at[tokens_at(s * blk, 1 - core)], place, jo_send.at[s, a], jo_recv.at[s, a], partner)
            closing.append((landed, launch(copy, s < jobs, s < jobs)))
            closing.append((done, local(src.at[tokens_at(s * blk, core)], place, jo_local.at[s, a], s < jobs)))
    for c in range(chips - 1):
        busy = c * groups < jobs
        owner = CORES * jnp.where(chip == 0, 1 + c, chips - 1) + core
        copy = remote(jl.at[c, 1 - core], lse_out.at[owner], jl_send.at[c], jl_recv.at[c], partner)
        closing.append((landed, launch(copy, busy, busy)))
        closing.append((done, local(jl.at[c, core], lse_out.at[owner], jl_local.at[c], busy)))

    out_arrays = ((ob, o_out, wide), (dqb, dq_out, wide), (dkb, dk_out, dim), (dvb, dv_out, dim))

    def out_copy(g, offset, a):
        src, dst, width = out_arrays[a]
        target = lax.rem(me + offset, n)
        at = lax.rem(offset + n - 1, n)
        return remote(src.at[g, row_of(target)], dst.at[:, column_of(me * groups + g, width)], out_send.at[g, at, a], out_recv.at[g, at, a], peer(offset))

    def own_copy(g, a):
        src, dst, width = out_arrays[a]
        return pltpu.make_async_copy(src.at[g, row_of(me)], dst.at[:, column_of(me * groups + g, width)], out_local.at[g, a])

    def head_compute(g):
        def key(j):
            return kb[g, block_of(j), :]

        def value(j):
            return vb[g, block_of(j), :]

        def lanes(r):
            return slice(r * dim, (r + 1) * dim)

        def prep(j, _):
            prepare(j, key, value)
            return 0

        lax.fori_loop(0, chips, prep, 0)

        def row(step, _):
            i = chips - 1 - step
            rows = block_of(i)

            def put_lse(r, t, x):
                lseb[i * CORES + t, pl.ds(g * ratio + r, 1), :] = x

            def put_out(r, x):
                ob[g, rows, lanes(r)] = x

            def put_dq(r, x):
                dqb[g, rows, lanes(r)] = x

            block(i, key, value, lambda r: qb[g, rows, lanes(r)], lambda r: gb[g, rows, lanes(r)], put_lse, put_out, put_dq)
            dkb[g, rows, :] = (dk_acc[rows, :] * scale).astype(BF16)
            dvb[g, rows, :] = dv_acc[rows, :].astype(BF16)
            early = True if g < groups - 1 else (chip == 0) | ((i < chips - 1) != (chip == chips - 1))
            for t in range(CORES):
                target = i * CORES + t
                for a in range(4):
                    pl.when((target != me) & early)(out_copy(g, lax.rem(target + n - me, n), a).start)
                    pl.when(target == me)(own_copy(g, a).start)
            return 0

        lax.fori_loop(0, chips - first_row(chip), row, 0)
        for b in range(JOB_CHIPS):
            @pl.when(b < first_row(chip))
            def _():
                o_part[g, b, 0] = dk_acc[b * blk:(b + 1) * blk, :] * scale
                o_part[g, b, 1] = dv_acc[b * blk:(b + 1) * blk, :]

    early_waits = []
    late_waits = []
    for g in range(groups):
        last = g == groups - 1
        waits = late_waits if last else early_waits
        for offset in range(n):
            for a in range(4):
                (landed if offset else done)(arrived[g, offset, a])
        head_compute(g)
        for b in range(JOB_CHIPS):
            slot = (chip - 1) * groups + g if b == 0 else g
            sends = b < first_row(chip)
            slot = jnp.where(sends, slot, 0)
            copy = remote(o_part.at[g, b], j_recv.at[slot], o_part_send.at[g, b], part_recv.at[slot], {"cp": CORES * b + core})
            launch(copy, sends)
        for offset in range(1, n):
            target = lax.rem(me + offset, n)
            target_chip = lax.div(target, CORES)
            sends = target_chip >= first_row(chip)
            receives = chip >= first_row(lax.div(lax.rem(me + n - offset, n), CORES))
            for a in range(4):
                copy = out_copy(g, offset, a)
                if last:
                    pl.when(sends & ((target_chip >= chips - 1) != (chip == chips - 1)) & (chip > 0))(copy.start)
                waits.append((send_done, (copy, sends)))
                waits.append((landed, (copy, receives)))
        for a in range(4):
            waits.append((done, (own_copy(g, a), None)))

    for offset in range(1, n):
        target = lax.rem(me + offset, n)
        sends = lax.div(target, CORES) >= first_row(chip)
        receives = chip >= first_row(lax.div(lax.rem(me + n - offset, n), CORES))
        copy = remote(lseb.at[target], lse_out.at[me], lse_send.at[offset - 1], lse_recv.at[offset - 1], peer(offset))
        pl.when(sends)(copy.start)
        late_waits.append((send_done, (copy, sends)))
        late_waits.append((landed, (copy, receives)))
    late_waits.append((done, local(lseb.at[me], lse_out.at[me], lse_local)))

    for wait, entry in closing + pending + early_waits:
        wait(entry)

    def total_of(s):
        tail = s - (chips - 2) * groups
        rows = pl.ds(pl.multiple_of(job_rows(s), blk), blk)
        for a, dst in enumerate((jk, jv)):
            if tail >= 0:
                @pl.when(chip == 0)
                def _():
                    j_own[s, a] += j_recv[slots + tail, a]

            dst[rows, :] = (j_own[s, a] + j_recv[s, a]).astype(BF16)

    final = []
    for g in range(groups):
        if g == groups - 1:
            for wait, entry in late_waits:
                wait(entry)
        for s in range(g, slots + groups, groups):
            wanted = chip <= 1 if s < groups else chip == 0
            copy = remote(j_part.at[0], j_recv.at[s], j_part_send.at[0], part_recv.at[s], partner)
            landed((copy, wanted))
        for s in range(g, slots, groups):
            pl.when(s < jobs)(functools.partial(total_of, s))
        for s in range(g, slots, groups):
            for a, (src, dst) in enumerate(((jk, dk_out), (jv, dv_out))):
                place = dst.at[:, column_of(job_head(s, core), dim)]
                base = job_rows(s)
                copy = remote(src.at[tokens_at(base, 1 - core)], place, fin_send.at[s, a], fin_recv.at[s, a], partner)
                pl.when(s < jobs)(copy.start)
                final.append((send_done, (copy, s < jobs)))
                final.append((landed, (copy, s < jobs)))
                final.append((done, local(src.at[tokens_at(base, core)], place, fin_local.at[s, a], s < jobs)))
    for wait, entry in final:
        wait(entry)


def solution(mesh):
    n = mesh.shape["cp"]

    def attention_shard(queries, keys, values, out_grad):
        batch, tokens, heads, dim = queries.shape
        kv_heads = keys.shape[2]
        ratio = heads // kv_heads
        groups = kv_heads // n
        total = n * tokens
        wide = ratio * dim
        blk = CORES * tokens
        slots = (n // CORES - 1) * groups
        stats = -(-groups * ratio // 8) * 8

        def flat(x):
            return x.reshape(tokens, x.shape[2], dim)

        any_space = pl.BlockSpec(memory_space=pl.ANY)
        vmem = pltpu.VMEM
        dma = pltpu.SemaphoreType.DMA
        out, dq, dk, dv, lse = pl.pallas_call(
            functools.partial(attention_kernel, n, groups, ratio, tokens, dim),
            out_shape=(
                jax.ShapeDtypeStruct((tokens, heads * dim), BF16),
                jax.ShapeDtypeStruct((tokens, heads * dim), BF16),
                jax.ShapeDtypeStruct((tokens, kv_heads * dim), BF16),
                jax.ShapeDtypeStruct((tokens, kv_heads * dim), BF16),
                jax.ShapeDtypeStruct((n, stats, tokens), F32),
            ),
            in_specs=[any_space] * 4,
            out_specs=(any_space,) * 5,
            scratch_shapes=[
                vmem((groups, total, wide), BF16),
                vmem((groups, total, dim), BF16),
                vmem((groups, total, dim), BF16),
                vmem((groups, total, wide), BF16),
                vmem((groups, total, wide), BF16),
                vmem((groups, total, wide), BF16),
                vmem((groups, total, dim), BF16),
                vmem((groups, total, dim), BF16),
                vmem((n, stats, tokens), F32),
                vmem((total, ratio * blk), F32),
                vmem((total, dim), F32),
                vmem((total, dim), F32),
                vmem((dim, total), BF16),
                vmem((dim, total), BF16),
                vmem((dim, ratio * blk), F32),
                vmem((ratio * blk, dim), BF16),
                vmem((ratio * blk, dim), BF16),
                vmem((tokens, heads, dim), BF16),
                vmem((tokens, kv_heads, dim), BF16),
                vmem((tokens, kv_heads, dim), BF16),
                vmem((tokens, heads, dim), BF16),
                vmem((kv_heads, tokens, wide), BF16),
                vmem((kv_heads, tokens, dim), BF16),
                vmem((kv_heads, tokens, dim), BF16),
                vmem((kv_heads, tokens, wide), BF16),
                vmem((tokens // 2 * (heads + 8), dim), F32),
                vmem((slots * blk, wide), BF16),
                vmem((slots * blk, dim), BF16),
                vmem((slots * blk, dim), BF16),
                vmem((slots * blk, wide), BF16),
                vmem((n // CORES - 1, CORES, stats, tokens), F32),
                vmem((slots, 2, blk, dim), F32),
                vmem((groups, 2, blk, dim), F32),
                vmem((slots + groups, 2, blk, dim), F32),
                vmem((groups, JOB_CHIPS, 2, blk, dim), F32),
                dma((4,)),
                dma((groups, n - 1, 4)),
                dma((groups, n - 1, 4)),
                dma((groups, n, 4)),
                dma((groups, n, 4)),
                dma((n - 1,)),
                dma((n - 1,)),
                dma((groups, 4)),
                dma((groups, 4)),
                dma,
                dma((slots, 4)),
                dma((slots, 4)),
                dma((slots, 4)),
                dma((CORES, groups, 2)),
                dma((CORES, groups, 2)),
                dma((slots, 2)),
                dma((slots, 2)),
                dma((slots, 2)),
                dma((n // CORES - 1,)),
                dma((n // CORES - 1,)),
                dma((n // CORES - 1,)),
                dma((groups, JOB_CHIPS)),
                dma((groups,)),
                dma((slots + groups,)),
                dma((slots, 2)),
                dma((slots, 2)),
                dma((slots, 2)),
            ],
            compiler_params=pltpu.CompilerParams(collective_id=0, has_side_effects=True, vmem_limit_bytes=62 * 2**20),
            name="heads_attention",
        )(flat(queries), flat(keys), flat(values), flat(out_grad))
        shape = (batch, tokens, heads, dim)
        kv_shape = (batch, tokens, kv_heads, dim)
        row_lse = lse[:, :groups * ratio, :].reshape(batch, heads, tokens)
        return out.reshape(shape), row_lse, dq.reshape(shape), dk.reshape(kv_shape), dv.reshape(kv_shape)

    seq_spec = P("dp", "cp")
    return jax.shard_map(attention_shard, mesh=mesh, in_specs=(seq_spec,) * 4, out_specs=(seq_spec, P("dp", None, "cp"), seq_spec, seq_spec, seq_spec), check_vma=False)
```

```python
import functools

import jax
import jax.numpy as jnp
from jax import lax
from jax.experimental import pallas as pl
from jax.experimental.pallas import tpu as pltpu
from jax.sharding import PartitionSpec as P

MESH = pl.DeviceIdType.MESH
F32 = jnp.float32
BF16 = jnp.bfloat16
NT = (((1,), (1,)), ((), ()))
CORES = 2
JOB_CHIPS = 2


def attention_kernel(n, groups, ratio, tokens, dim, q_in, k_in, v_in, g_in, o_out, dq_out, dk_out, dv_out, lse_out, qb, kb, vb, gb, ob, dqb, dkb, dvb, lseb, s_scr, dk_acc, dv_acc, kt, vt, t_scr, q_cat, g_cat, q_stage, k_stage, v_stage, q_send, k_send, v_send, g_send, f_scr, jq, jk, jv, jg, jl, j_own, j_part, j_recv, o_part, stage_sem, in_send, in_recv, out_send, out_recv, lse_send, lse_recv, in_local, out_local, lse_local, ji_send, ji_recv, ji_local, jk_send, jk_recv, jo_send, jo_recv, jo_local, jl_send, jl_recv, jl_local, o_part_send, j_part_send, part_recv, fin_send, fin_recv, fin_local):
    me = lax.axis_index("cp")
    chip = lax.div(me, CORES)
    core = lax.rem(me, CORES)
    chips = n // CORES
    scale = dim ** -0.5
    wide = ratio * dim
    blk = CORES * tokens
    cols = ratio * blk
    rows_total = chips * blk
    slots = (chips - 1) * groups
    jobs = jnp.where(chip == 0, slots, jnp.where(chip == 1, groups, 0))

    def first_row(owner_chip):
        return lax.div(owner_chip + 1, 2)

    def peer(offset):
        return {"cp": lax.rem(me + offset, n)}

    partner = {"cp": me + 1 - 2 * core}

    def row_of(device):
        return pl.ds(pl.multiple_of(device * tokens, tokens), tokens)

    def block_of(index):
        return pl.ds(pl.multiple_of(index * blk, blk), blk)

    def column_of(head, width):
        return pl.ds(pl.multiple_of(head * width, width), width)

    def remote(src, dst, send_sem, recv_sem, device):
        return pltpu.make_async_remote_copy(src_ref=src, dst_ref=dst, send_sem=send_sem, recv_sem=recv_sem, device_id=device, device_id_type=MESH)

    pending = []

    def launch(copy, sends=None, receives=None):
        if sends is None:
            copy.start()
        else:
            pl.when(sends)(copy.start)
        pending.append((send_done, (copy, sends)))
        return (copy, receives)

    def landed(entry):
        copy, receives = entry
        if receives is None:
            copy.wait_recv()
        else:
            pl.when(receives)(copy.wait_recv)

    def send_done(entry):
        copy, sends = entry
        if sends is None:
            copy.wait_send()
        else:
            pl.when(sends)(copy.wait_send)

    def local(src, dst, sem, cond=None):
        copy = pltpu.make_async_copy(src, dst, sem)
        if cond is None:
            copy.start()
        else:
            pl.when(cond)(copy.start)
        return (copy, cond)

    def done(entry):
        copy, cond = entry
        if cond is None:
            copy.wait()
        else:
            pl.when(cond)(copy.wait)

    stage_copies = [local(src, dst, stage_sem.at[a]) for a, (src, dst) in enumerate(((k_in, k_stage), (v_in, v_stage), (q_in, q_stage)))]

    barrier = pltpu.get_barrier_semaphore()
    for offset in range(1, n):
        pl.semaphore_signal(barrier, inc=1, device_id=peer(offset), device_id_type=MESH)

    def split_heads(stage, send):
        heads = stage.shape[1]
        per = heads // send.shape[0]
        pad = heads + 8
        step = 16
        half = tokens // 2
        for part in range(2):
            def widen(t, _):
                base = t * step
                piece = stage[pl.ds(part * half + base, step)].astype(F32)
                for u in range(step):
                    f_scr[pl.ds(pl.multiple_of((base + u) * pad, 8), heads), :] = piece[u]
                return 0

            lax.fori_loop(0, half // step, widen, 0)

            def gather(h, _):
                for r in range(per):
                    send[h, part * half:(part + 1) * half, r * dim:(r + 1) * dim] = f_scr[pl.ds(h * per + r, half, stride=pad), :].astype(BF16)
                return 0

            lax.fori_loop(0, send.shape[0], gather, 0)

    in_arrays = ((k_send, kb), (v_send, vb), (q_send, qb), (g_send, gb))
    job_arrays = ((k_send, jk), (v_send, jv), (q_send, jq), (g_send, jg))
    arrived = {}
    job_arrived = []

    def send_in(g, a):
        src, dst = in_arrays[a]
        for offset in range(1, n):
            target = lax.rem(me + offset, n)
            sends = receives = None
            if a >= 2:
                sends = chip >= first_row(lax.div(target, CORES))
                receives = lax.div(lax.rem(me + n - offset, n), CORES) >= first_row(chip)
            copy = remote(src.at[target * groups + g], dst.at[g, row_of(me)], in_send.at[g, offset - 1, a], in_recv.at[g, offset - 1, a], peer(offset))
            arrived[g, offset, a] = launch(copy, sends, receives)
        arrived[g, 0, a] = local(src.at[me * groups + g], dst.at[g, row_of(me)], in_local.at[g, a])

    def job_head(slot, which_core):
        owner_chip = jnp.where(chip == 0, 1 + slot // groups, chips - 1)
        return (CORES * owner_chip + which_core) * groups + slot % groups

    def job_rows(slot):
        return (slot * (chip + 1) + chip) * blk

    def tokens_at(base, which_core):
        return pl.ds(pl.multiple_of(base + which_core * tokens, tokens), tokens)

    def send_job(a):
        src, dst = job_arrays[a]
        for s in range(slots):
            base = job_rows(s) if a < 2 else s * blk
            place = dst.at[tokens_at(base, core)]
            copy = remote(src.at[job_head(s, 1 - core)], place, ji_send.at[s, a], ji_recv.at[s, a], partner)
            job_arrived.append((landed, launch(copy, s < jobs, s < jobs)))
            job_arrived.append((done, local(src.at[job_head(s, core)], place, ji_local.at[s, a], s < jobs)))

    done(stage_copies[0])
    split_heads(k_stage, k_send)
    done(stage_copies[1])
    pl.semaphore_wait(barrier, n - 1)
    send_in(0, 0)
    split_heads(v_stage, v_send)
    send_job(0)
    for k in range(CORES):
        for g in range(groups):
            for a in range(2):
                src, dst = job_arrays[a]
                copy = remote(
                    src.at[(CORES * (chips - 1) + k) * groups + g],
                    dst.at[tokens_at(g * 2 * blk, core)],
                    jk_send.at[k, g, a],
                    jk_recv.at[core, g, a],
                    {"cp": CORES + k},
                )
                launch(copy, chip == 0)
    done(stage_copies[2])
    split_heads(q_stage, q_send)
    cotangents = local(g_in, q_stage, stage_sem.at[3])
    send_job(1)
    send_job(2)
    send_in(0, 1)
    done(cotangents)
    split_heads(q_stage, g_send)
    send_in(0, 2)
    send_job(3)
    send_in(0, 3)
    for g in range(1, groups):
        for a in range(4):
            send_in(g, a)

    key_pos = lax.broadcasted_iota(jnp.int32, (blk, blk), 0)
    query_pos = lax.broadcasted_iota(jnp.int32, (blk, blk), 1)

    def fold(x, op):
        return op(x.reshape(blk // 8, 8, cols), axis=0)

    def prepare(j, key, value):
        rows = block_of(j)
        kt[:, rows] = jnp.transpose(key(j).astype(F32)).astype(BF16)
        vt[:, rows] = jnp.transpose(value(j).astype(F32)).astype(BF16)
        dk_acc[rows, :] = jnp.zeros((blk, dim), F32)
        dv_acc[rows, :] = jnp.zeros((blk, dim), F32)

    def block(i, key, value, query, cotangent, put_lse, put_out, put_dq):
        rows_i = block_of(i)
        for r in range(ratio):
            q_cat[r * blk:(r + 1) * blk, :] = query(r)
            g_cat[r * blk:(r + 1) * blk, :] = cotangent(r)

        def score(j, top):
            s = lax.dot_general(key(j), q_cat[...], NT, preferred_element_type=F32)
            s_scr[block_of(j), :] = s
            return jnp.maximum(top, fold(s, jnp.max))

        top = lax.fori_loop(0, i, score, jnp.full((8, cols), -jnp.inf, F32))
        s = lax.dot_general(key(i), q_cat[...], NT, preferred_element_type=F32)
        keep = jnp.concatenate([key_pos <= query_pos] * ratio, axis=1)
        s = jnp.where(keep, s, -jnp.inf)
        s_scr[rows_i, :] = s
        top = jnp.max(jnp.maximum(top, fold(s, jnp.max)), axis=0, keepdims=True)

        def weigh(j, total):
            rows = block_of(j)
            p = jnp.exp((s_scr[rows, :] - top) * scale)
            s_scr[rows, :] = p
            return total + fold(p, jnp.sum)

        total = lax.fori_loop(0, i + 1, weigh, jnp.zeros((8, cols), F32))
        total = jnp.sum(total, axis=0, keepdims=True)
        inv = 1.0 / total
        lse = top * scale + jnp.log(total)
        for r in range(ratio):
            for t in range(CORES):
                at = r * blk + t * tokens
                put_lse(r, t, lse[:, at:at + tokens])
        t_scr[...] = jnp.zeros((dim, cols), F32)

        def outputs(j, _):
            rows = block_of(j)
            p_low = (s_scr[rows, :] * inv).astype(BF16)
            t_scr[...] += jnp.dot(vt[:, rows], p_low, preferred_element_type=F32)
            dv_acc[rows, :] += jnp.dot(p_low, g_cat[...], preferred_element_type=F32)
            return 0

        lax.fori_loop(0, i + 1, outputs, 0)
        out = jnp.transpose(t_scr[...]).astype(BF16)
        for r in range(ratio):
            put_out(r, out[r * blk:(r + 1) * blk])
        delta = jnp.sum(jnp.transpose(g_cat[...].astype(F32) * out.astype(F32)), axis=0, keepdims=True)
        t_scr[...] = jnp.zeros((dim, cols), F32)

        def gradients(j, _):
            rows = block_of(j)
            dp = lax.dot_general(value(j), g_cat[...], NT, preferred_element_type=F32)
            ds = ((s_scr[rows, :] * inv) * (dp - delta)).astype(BF16)
            t_scr[...] += jnp.dot(kt[:, rows], ds, preferred_element_type=F32)
            dk_acc[rows, :] += jnp.dot(ds, q_cat[...], preferred_element_type=F32)
            return 0

        lax.fori_loop(0, i + 1, gradients, 0)
        dq = jnp.transpose(t_scr[...] * scale).astype(BF16)
        for r in range(ratio):
            put_dq(r, dq[r * blk:(r + 1) * blk])

    for wait, entry in job_arrived:
        wait(entry)
    for j in range(CORES):
        for g in range(groups):
            for a in range(2):
                src, dst = job_arrays[a]
                copy = remote(src.at[0], dst.at[tokens_at(g * 2 * blk, j)], jk_send.at[0, g, a], jk_recv.at[j, g, a], partner)
                landed((copy, chip == 1))

    def job(s, _):
        def key(j):
            return jk[pl.ds(pl.multiple_of((s * (chip + 1) + j) * blk, blk), blk), :]

        def value(j):
            return jv[pl.ds(pl.multiple_of((s * (chip + 1) + j) * blk, blk), blk), :]

        def lanes(r):
            return slice(r * dim, (r + 1) * dim)

        rows = block_of(s)
        group = lax.div(s, groups)
        stat = lax.rem(s, groups) * ratio

        def put_lse(r, t, x):
            jl[group, t, pl.ds(stat + r, 1), :] = x

        def put_out(r, x):
            jq[rows, lanes(r)] = x

        def put_dq(r, x):
            jg[rows, lanes(r)] = x

        def prep(j, _):
            prepare(j, key, value)
            return 0

        lax.fori_loop(0, chip + 1, prep, 0)
        block(chip, key, value, lambda r: jq[rows, lanes(r)], lambda r: jg[rows, lanes(r)], put_lse, put_out, put_dq)
        own = block_of(chip)
        j_own[s, 0] = dk_acc[own, :] * scale
        j_own[s, 1] = dv_acc[own, :]

        @pl.when(chip == 1)
        def _():
            j_part[s, 0] = dk_acc[0:blk, :] * scale
            j_part[s, 1] = dv_acc[0:blk, :]

        return 0

    lax.fori_loop(0, jobs, job, 0)

    closing = []
    for g in range(groups):
        copy = remote(j_part.at[g], j_recv.at[slots + g], j_part_send.at[g], part_recv.at[slots + g], {"cp": core})
        launch(copy, chip == 1)
    for s in range(slots):
        for a, (src, dst) in enumerate(((jq, o_out), (jg, dq_out))):
            place = dst.at[:, column_of(job_head(s, core), wide)]
            copy = remote(src.at[tokens_at(s * blk, 1 - core)], place, jo_send.at[s, a], jo_recv.at[s, a], partner)
            closing.append((landed, launch(copy, s < jobs, s < jobs)))
            closing.append((done, local(src.at[tokens_at(s * blk, core)], place, jo_local.at[s, a], s < jobs)))
    for c in range(chips - 1):
        busy = c * groups < jobs
        owner = CORES * jnp.where(chip == 0, 1 + c, chips - 1) + core
        copy = remote(jl.at[c, 1 - core], lse_out.at[owner], jl_send.at[c], jl_recv.at[c], partner)
        closing.append((landed, launch(copy, busy, busy)))
        closing.append((done, local(jl.at[c, core], lse_out.at[owner], jl_local.at[c], busy)))

    out_arrays = ((ob, o_out, wide), (dqb, dq_out, wide), (dkb, dk_out, dim), (dvb, dv_out, dim))

    def out_copy(g, offset, a):
        src, dst, width = out_arrays[a]
        target = lax.rem(me + offset, n)
        at = lax.rem(offset + n - 1, n)
        return remote(src.at[g, row_of(target)], dst.at[:, column_of(me * groups + g, width)], out_send.at[g, at, a], out_recv.at[g, at, a], peer(offset))

    def own_copy(g, a):
        src, dst, width = out_arrays[a]
        return pltpu.make_async_copy(src.at[g, row_of(me)], dst.at[:, column_of(me * groups + g, width)], out_local.at[g, a])

    def head_compute(g):
        def key(j):
            return kb[g, block_of(j), :]

        def value(j):
            return vb[g, block_of(j), :]

        def lanes(r):
            return slice(r * dim, (r + 1) * dim)

        def prep(j, _):
            prepare(j, key, value)
            return 0

        lax.fori_loop(0, chips, prep, 0)

        def row(step, _):
            i = chips - 1 - step
            rows = block_of(i)

            def put_lse(r, t, x):
                lseb[i * CORES + t, pl.ds(g * ratio + r, 1), :] = x

            def put_out(r, x):
                ob[g, rows, lanes(r)] = x

            def put_dq(r, x):
                dqb[g, rows, lanes(r)] = x

            block(i, key, value, lambda r: qb[g, rows, lanes(r)], lambda r: gb[g, rows, lanes(r)], put_lse, put_out, put_dq)
            dkb[g, rows, :] = (dk_acc[rows, :] * scale).astype(BF16)
            dvb[g, rows, :] = dv_acc[rows, :].astype(BF16)
            early = True if g < groups - 1 else (chip == 0) | ((i < chips - 1) != (chip == chips - 1))
            for t in range(CORES):
                target = i * CORES + t
                for a in range(4):
                    pl.when((target != me) & early)(out_copy(g, lax.rem(target + n - me, n), a).start)
                    pl.when(target == me)(own_copy(g, a).start)
            return 0

        lax.fori_loop(0, chips - first_row(chip), row, 0)
        for b in range(JOB_CHIPS):
            @pl.when(b < first_row(chip))
            def _():
                o_part[g, b, 0] = dk_acc[b * blk:(b + 1) * blk, :] * scale
                o_part[g, b, 1] = dv_acc[b * blk:(b + 1) * blk, :]

    early_waits = []
    late_waits = []
    for g in range(groups):
        last = g == groups - 1
        waits = late_waits if last else early_waits
        for offset in range(n):
            for a in range(4):
                (landed if offset else done)(arrived[g, offset, a])
        head_compute(g)
        for b in range(JOB_CHIPS):
            slot = (chip - 1) * groups + g if b == 0 else g
            sends = b < first_row(chip)
            slot = jnp.where(sends, slot, 0)
            copy = remote(o_part.at[g, b], j_recv.at[slot], o_part_send.at[g, b], part_recv.at[slot], {"cp": CORES * b + core})
            launch(copy, sends)
        for offset in range(1, n):
            target = lax.rem(me + offset, n)
            target_chip = lax.div(target, CORES)
            sends = target_chip >= first_row(chip)
            receives = chip >= first_row(lax.div(lax.rem(me + n - offset, n), CORES))
            for a in range(4):
                copy = out_copy(g, offset, a)
                if last:
                    pl.when(sends & ((target_chip >= chips - 1) != (chip == chips - 1)) & (chip > 0))(copy.start)
                waits.append((send_done, (copy, sends)))
                waits.append((landed, (copy, receives)))
        for a in range(4):
            waits.append((done, (own_copy(g, a), None)))

    for offset in range(1, n):
        target = lax.rem(me + offset, n)
        sends = lax.div(target, CORES) >= first_row(chip)
        receives = chip >= first_row(lax.div(lax.rem(me + n - offset, n), CORES))
        copy = remote(lseb.at[target], lse_out.at[me], lse_send.at[offset - 1], lse_recv.at[offset - 1], peer(offset))
        pl.when(sends)(copy.start)
        late_waits.append((send_done, (copy, sends)))
        late_waits.append((landed, (copy, receives)))
    late_waits.append((done, local(lseb.at[me], lse_out.at[me], lse_local)))

    for wait, entry in closing + pending + early_waits:
        wait(entry)

    def total_of(s):
        tail = s - (chips - 2) * groups
        rows = pl.ds(pl.multiple_of(job_rows(s), blk), blk)
        for a, dst in enumerate((jk, jv)):
            if tail >= 0:
                @pl.when(chip == 0)
                def _():
                    j_own[s, a] += j_recv[slots + tail, a]

            dst[rows, :] = (j_own[s, a] + j_recv[s, a]).astype(BF16)

    final = []
    for g in range(groups):
        for s in range(g, slots + groups, groups):
            wanted = chip <= 1 if s < groups else chip == 0
            copy = remote(j_part.at[0], j_recv.at[s], j_part_send.at[0], part_recv.at[s], partner)
            landed((copy, wanted))
        for s in range(g, slots, groups):
            pl.when(s < jobs)(functools.partial(total_of, s))
        for s in range(g, slots, groups):
            for a, (src, dst) in enumerate(((jk, dk_out), (jv, dv_out))):
                place = dst.at[:, column_of(job_head(s, core), dim)]
                base = job_rows(s)
                copy = remote(src.at[tokens_at(base, 1 - core)], place, fin_send.at[s, a], fin_recv.at[s, a], partner)
                pl.when(s < jobs)(copy.start)
                final.append((send_done, (copy, s < jobs)))
                final.append((landed, (copy, s < jobs)))
                final.append((done, local(src.at[tokens_at(base, core)], place, fin_local.at[s, a], s < jobs)))
    for wait, entry in late_waits + final:
        wait(entry)


def solution(mesh):
    n = mesh.shape["cp"]

    def attention_shard(queries, keys, values, out_grad):
        batch, tokens, heads, dim = queries.shape
        kv_heads = keys.shape[2]
        ratio = heads // kv_heads
        groups = kv_heads // n
        total = n * tokens
        wide = ratio * dim
        blk = CORES * tokens
        slots = (n // CORES - 1) * groups
        stats = -(-groups * ratio // 8) * 8

        def flat(x):
            return x.reshape(tokens, x.shape[2], dim)

        any_space = pl.BlockSpec(memory_space=pl.ANY)
        vmem = pltpu.VMEM
        dma = pltpu.SemaphoreType.DMA
        out, dq, dk, dv, lse = pl.pallas_call(
            functools.partial(attention_kernel, n, groups, ratio, tokens, dim),
            out_shape=(
                pltpu.VMEM((tokens, heads * dim), BF16),
                pltpu.VMEM((tokens, heads * dim), BF16),
                pltpu.VMEM((tokens, kv_heads * dim), BF16),
                pltpu.VMEM((tokens, kv_heads * dim), BF16),
                pltpu.VMEM((n, stats, tokens), F32),
            ),
            in_specs=[any_space] * 4,
            out_specs=(pl.BlockSpec(memory_space=pltpu.VMEM),) * 5,
            scratch_shapes=[
                vmem((groups, total, wide), BF16),
                vmem((groups, total, dim), BF16),
                vmem((groups, total, dim), BF16),
                vmem((groups, total, wide), BF16),
                vmem((groups, total, wide), BF16),
                vmem((groups, total, wide), BF16),
                vmem((groups, total, dim), BF16),
                vmem((groups, total, dim), BF16),
                vmem((n, stats, tokens), F32),
                vmem((total, ratio * blk), F32),
                vmem((total, dim), F32),
                vmem((total, dim), F32),
                vmem((dim, total), BF16),
                vmem((dim, total), BF16),
                vmem((dim, ratio * blk), F32),
                vmem((ratio * blk, dim), BF16),
                vmem((ratio * blk, dim), BF16),
                vmem((tokens, heads, dim), BF16),
                vmem((tokens, kv_heads, dim), BF16),
                vmem((tokens, kv_heads, dim), BF16),
                vmem((kv_heads, tokens, wide), BF16),
                vmem((kv_heads, tokens, dim), BF16),
                vmem((kv_heads, tokens, dim), BF16),
                vmem((kv_heads, tokens, wide), BF16),
                vmem((tokens // 2 * (heads + 8), dim), F32),
                vmem((slots * blk, wide), BF16),
                vmem((slots * blk, dim), BF16),
                vmem((slots * blk, dim), BF16),
                vmem((slots * blk, wide), BF16),
                vmem((n // CORES - 1, CORES, stats, tokens), F32),
                vmem((slots, 2, blk, dim), F32),
                vmem((groups, 2, blk, dim), F32),
                vmem((slots + groups, 2, blk, dim), F32),
                vmem((groups, JOB_CHIPS, 2, blk, dim), F32),
                dma((4,)),
                dma((groups, n - 1, 4)),
                dma((groups, n - 1, 4)),
                dma((groups, n, 4)),
                dma((groups, n, 4)),
                dma((n - 1,)),
                dma((n - 1,)),
                dma((groups, 4)),
                dma((groups, 4)),
                dma,
                dma((slots, 4)),
                dma((slots, 4)),
                dma((slots, 4)),
                dma((CORES, groups, 2)),
                dma((CORES, groups, 2)),
                dma((slots, 2)),
                dma((slots, 2)),
                dma((slots, 2)),
                dma((n // CORES - 1,)),
                dma((n // CORES - 1,)),
                dma((n // CORES - 1,)),
                dma((groups, JOB_CHIPS)),
                dma((groups,)),
                dma((slots + groups,)),
                dma((slots, 2)),
                dma((slots, 2)),
                dma((slots, 2)),
            ],
            compiler_params=pltpu.CompilerParams(collective_id=0, has_side_effects=True, vmem_limit_bytes=57 * 2**20),
            name="heads_attention",
        )(flat(queries), flat(keys), flat(values), flat(out_grad))
        shape = (batch, tokens, heads, dim)
        kv_shape = (batch, tokens, kv_heads, dim)
        row_lse = lse[:, :groups * ratio, :].reshape(batch, heads, tokens)
        return out.reshape(shape), row_lse, dq.reshape(shape), dk.reshape(kv_shape), dv.reshape(kv_shape)

    seq_spec = P("dp", "cp")
    return jax.shard_map(attention_shard, mesh=mesh, in_specs=(seq_spec,) * 4, out_specs=(seq_spec, P("dp", None, "cp"), seq_spec, seq_spec, seq_spec), check_vma=False)
```
